32 devices in a mesh: req: 8 (over y, x, core), kv: 4 (over z).
Axes of the slice: x: 2, y: 2, z: 4, core: 2. Of those that a mesh axis runs over, the one named last changes fastest.
Arguments:
- queries: bfloat16 [32, 4096], P(('req', 'kv')), may hold values from -16 to 16
- paged_key_cache: bfloat16 [192, 128, 1024], P(('req', 'kv')), may hold values from -8 to 8
- paged_value_cache: bfloat16 [192, 128, 1024], P(('req', 'kv')), may hold values from -6 to 6
- page_request: int32 [192], P(('req', 'kv')), may hold values from 0 to 31, as said below
- page_number: int32 [192], P(('req', 'kv')), may hold values from 0 to 7, as said below
- lengths: int32 [32], replicated, may hold values from 1 to 1024, as said below
Outputs:
- attended: bfloat16 [32, 4096], P(('req', 'kv'))
The draws below stay inside these ranges and needn't reach their ends.
Inputs may be any that keep to these rules, and one draw needn't show every extreme that they name: `page_request`: every request has 1 to 8 pages and some request exactly 8; the 6 slots of one device hold pages of requests r with 6 different values of r // 4. `page_number`: the pages of one request are numbered 0, 1, 2 and so on without gaps, each number once. `lengths`: a request with n pages has a length from (n - 1) * 128 + 1 to n * 128.
All inputs are finite; a program needn't handle non-finite values.
Results may differ from the reference program's by a relative error of at most 0.0023.
Values may be sent and summed in bfloat16 or wider, within the bound.
A program may use at most 64 MiB of HBM per device.

```python
import jax
import jax.numpy as jnp
from jax import lax

HQ = 32
KEY_VALUE_HEADS = 8
HEAD_SIZE = 128
PAGE_TOKENS = 128
DEVICE_PAGES = 6
QUERY_PER_KV = 4
REQUESTS = 32
TOTAL_PAGES = 192
MOST_PAGES = 8
DEVICES = 32


def page_tables(key):
    base = jax.random.fold_in(key, 11)
    streams = jax.random.split(base, 7)
    relabel = jax.random.permutation(streams[0], REQUESTS).astype(jnp.int32)
    starts = jax.random.randint(streams[1], (REQUESTS,), 0, 1024).astype(jnp.int32)
    slopes = jax.random.randint(streams[2], (REQUESTS,), 1, 65).astype(jnp.int32)
    forced = relabel[0]
    starts = starts.at[forced].set(4096)
    slopes = slopes.at[forced].set(1)
    cells = REQUESTS * MOST_PAGES
    ranks = jnp.arange(MOST_PAGES, dtype=jnp.int32)
    ties = jax.random.permutation(streams[3], cells).astype(jnp.int32).reshape(REQUESTS, MOST_PAGES)
    score = (starts[:, None] - ranks[None, :] * slopes[:, None]) * cells + ties
    score = jnp.where(ranks[None, :] == 0, 2 ** 30, score).reshape(cells)
    order = jnp.argsort(-score)
    chosen = jnp.zeros((cells,), jnp.int32).at[order[:TOTAL_PAGES]].set(1)
    flat = jnp.arange(cells, dtype=jnp.int32)
    listing = jnp.argsort((1 - chosen) * cells + flat)[:TOTAL_PAGES].astype(jnp.int32)
    request_of = listing // MOST_PAGES
    number_of = listing % MOST_PAGES
    places = jnp.arange(TOTAL_PAGES, dtype=jnp.int32)
    shuffle = jax.random.permutation(streams[4], DEVICES).astype(jnp.int32)
    device = jnp.take(shuffle, places % DEVICES)
    offsets = jax.random.randint(streams[5], (DEVICES,), 0, DEVICE_PAGES).astype(jnp.int32)
    slot = (places // DEVICES + jnp.take(offsets, device)) % DEVICE_PAGES
    position = device * DEVICE_PAGES + slot
    owners = jnp.zeros((TOTAL_PAGES,), jnp.int32).at[position].set(request_of)
    numbers = jnp.zeros((TOTAL_PAGES,), jnp.int32).at[position].set(number_of)
    counts = jnp.sum(chosen.reshape(REQUESTS, MOST_PAGES), axis=1)
    extra = jax.random.randint(streams[6], (REQUESTS,), 1, PAGE_TOKENS + 1)
    request_lengths = ((counts - 1) * PAGE_TOKENS + extra).astype(jnp.int32)
    return (owners, numbers, request_lengths)


def draw_page_request(key, part):
    return page_tables(key)[0]


def draw_page_number(key, part):
    return page_tables(key)[1]


def draw_lengths(key, part):
    return page_tables(key)[2]


def draw_queries(key, part):
    random_noise = jax.random.normal(jax.random.fold_in(key, 21), (REQUESTS, HQ, HEAD_SIZE), jnp.float32)
    result = jnp.clip(2.5 * random_noise, -16.0, 16.0)
    return result.reshape(REQUESTS, HQ * HEAD_SIZE).astype(jnp.bfloat16)


def draw_paged_key_cache(key, part):
    random_noise = jnp.clip(jax.random.normal(jax.random.fold_in(key, 41), (TOTAL_PAGES, PAGE_TOKENS, KEY_VALUE_HEADS, HEAD_SIZE), jnp.float32), -6.0, 6.0)
    return random_noise.reshape(TOTAL_PAGES, PAGE_TOKENS, KEY_VALUE_HEADS * HEAD_SIZE).astype(jnp.bfloat16)


def level_of(stream_key, extent, cuts, least, top_value):
    gain = 1.0
    for axis_at, parts in cuts:
        draws = jax.random.uniform(jax.random.fold_in(jax.random.fold_in(stream_key, 6), axis_at), (parts,), jnp.float32, least / len(cuts), top_value / len(cuts))
        gain = gain * jnp.repeat(jnp.exp(draws), extent[axis_at] // parts).reshape((-1,) + (1,) * (len(extent) - 1 - axis_at))
    return gain


def noise(rng, shape, width, most, cuts=(), kind=jnp.bfloat16):
    drawn = width * jax.random.normal(rng, shape, jnp.float32)
    if cuts:
        drawn = drawn * level_of(rng, shape, cuts, -0.22, 0.18)
    return jnp.clip(drawn, -most, most).astype(kind)


def setup_inputs(seed: int = 0) -> dict:
    key_of = jax.random.split(jax.random.key(seed), 7)
    queries = draw_queries(jax.random.fold_in(key_of[6], 71), 0)
    paged_key_cache = draw_paged_key_cache(jax.random.fold_in(key_of[6], 71), 0)
    paged_value_cache = noise(key_of[2], (TOTAL_PAGES, PAGE_TOKENS, KEY_VALUE_HEADS * HEAD_SIZE), 1.0, 6.0, ((0, 32),))
    page_request = draw_page_request(jax.random.fold_in(key_of[6], 71), 0)
    page_number = draw_page_number(jax.random.fold_in(key_of[6], 71), 0)
    lengths = draw_lengths(jax.random.fold_in(key_of[6], 71), 0)
    return dict(queries=queries, paged_key_cache=paged_key_cache, paged_value_cache=paged_value_cache, page_request=page_request, page_number=page_number, lengths=lengths)


lowest = -1e30


def page_attention(gathered_query_rows, gathered_key_rows, gathered_value_rows, usable):
    token_count = gathered_query_rows.shape[0]
    query_single = gathered_query_rows.astype(jnp.float32).reshape(token_count, KEY_VALUE_HEADS, QUERY_PER_KV, HEAD_SIZE)
    key_single = gathered_key_rows.astype(jnp.float32).reshape(token_count, PAGE_TOKENS, KEY_VALUE_HEADS, HEAD_SIZE)
    value_single = gathered_value_rows.astype(jnp.float32).reshape(token_count, PAGE_TOKENS, KEY_VALUE_HEADS, HEAD_SIZE)
    scores = jnp.einsum("sgqd,stgd->sgqt", query_single, key_single, precision=lax.Precision.HIGHEST) * (HEAD_SIZE ** -0.5)
    scores = jnp.where(usable[:, None, None, :], scores, lowest)
    maxima = jnp.max(scores, axis=-1)
    weights = jnp.exp(scores - maxima[..., None])
    sums_exp = jnp.sum(weights, axis=-1)
    rounded = weights.astype(jnp.bfloat16).astype(jnp.float32)
    partial_out = jnp.einsum("sgqt,stgd->sgqd", rounded, value_single, precision=lax.Precision.HIGHEST)
    return maxima.reshape(token_count, HQ), sums_exp.reshape(token_count, HQ), partial_out.reshape(token_count, HQ * HEAD_SIZE)


def reference(queries, paged_key_cache, paged_value_cache, page_request, page_number, lengths):
    request_blocks = page_request.reshape(DEVICES, DEVICE_PAGES)
    number_blocks = page_number.reshape(DEVICES, DEVICE_PAGES)
    paged_key_blocks = paged_key_cache.reshape(DEVICES, DEVICE_PAGES, PAGE_TOKENS, KEY_VALUE_HEADS * HEAD_SIZE)
    paged_value_blocks = paged_value_cache.reshape(DEVICES, DEVICE_PAGES, PAGE_TOKENS, KEY_VALUE_HEADS * HEAD_SIZE)
    positions = jnp.arange(PAGE_TOKENS, dtype=jnp.int32)

    def per_block(block):
        owners, numbers, gathered_key_rows, gathered_value_rows = block
        gathered_query_rows = jnp.take(queries, owners, axis=0)
        limits = jnp.take(lengths, owners)
        usable = numbers[:, None] * PAGE_TOKENS + positions[None, :] < limits[:, None]
        return page_attention(gathered_query_rows, gathered_key_rows, gathered_value_rows, usable)

    maxima, sums_exp, partial_out = lax.map(per_block, (request_blocks, number_blocks, paged_key_blocks, paged_value_blocks))
    maxima = maxima.reshape(TOTAL_PAGES, HQ)
    sums_exp = sums_exp.reshape(TOTAL_PAGES, HQ)
    partial_out = partial_out.reshape(TOTAL_PAGES, HQ, HEAD_SIZE)
    request_max = jnp.full((REQUESTS, HQ), lowest, jnp.float32).at[page_request].max(maxima)
    factors = jnp.exp(maxima - jnp.take(request_max, page_request, axis=0))
    numerators = jnp.zeros((REQUESTS, HQ, HEAD_SIZE), jnp.float32).at[page_request].add(factors[:, :, None] * partial_out)
    denominators = jnp.zeros((REQUESTS, HQ), jnp.float32).at[page_request].add(factors * sums_exp)
    attended = numerators / denominators[:, :, None]
    return attended.reshape(REQUESTS, HQ * HEAD_SIZE).astype(jnp.bfloat16)
```

```python
import functools

import jax
import jax.numpy as jnp
from jax import lax
from jax.experimental import pallas as pl
from jax.experimental.pallas import tpu as pltpu
from jax.sharding import PartitionSpec as P

HQ = 32
KEY_VALUE_HEADS = 8
HEAD_SIZE = 128
QUERY_PER_KV = 4
CORES = 2
PAIR = 2 * QUERY_PER_KV

lowest = -1e30
MESH = pl.DeviceIdType.MESH


def partners(me, n):
    if n & (n - 1):
        return [lax.rem(me + d, n) for d in range(n)]
    found = []
    for d in range(n):
        place, bit = me, 1
        while bit < n:
            if d & bit:
                place = place + bit - 2 * bit * lax.rem(lax.div(me, bit), 2)
            bit *= 2
        found.append(place)
    return found


def diagonal_to_lanes(column, on_diagonal):
    return jnp.sum(jnp.where(on_diagonal, column, 0.0), axis=0, keepdims=True)


def lanes_to_column(row, on_diagonal):
    return jnp.sum(jnp.where(on_diagonal, row, 0.0), axis=1, keepdims=True)


def kernel(
    n_req, n_kv, group,
    owner_hbm, number_hbm, length_hbm, q_hbm, key_hbm, value_hbm, out_ref,
    owner_ref, number_ref, length_ref, q_ref, keys, values, q_rows, q_own, q_col, table, held, q_send, q_in,
    part_send, part_in, merged, merged_in,
    small_sem, page_sem, qs_sem, qr_sem, ts_sem, tr_sem, ds_sem, dr_sem, ps_sem, pr_sem, ms_sem, mr_sem,
):
    slots, page_tokens, _ = keys.shape
    n_chip = n_req // CORES
    my_req = lax.axis_index("req")
    my_kv = lax.axis_index("kv")
    my_chip = lax.div(my_req, CORES)
    core = lax.rem(my_req, CORES)
    is_hub = core == CORES - 1
    is_leaf = core < CORES - 1
    chip_peers = partners(my_chip, n_chip)
    kv_peers = partners(my_kv, n_kv)
    hub_of = [CORES * chip + CORES - 1 for chip in chip_peers]
    leaf_of = [CORES * chip for chip in chip_peers]

    barrier = pltpu.get_barrier_semaphore()

    @pl.when(is_hub)
    def _():
        for d in range(n_kv - 1, 0, -1):
            pl.semaphore_signal(barrier, inc=1, device_id=(hub_of[0], kv_peers[d]), device_id_type=MESH)
        for d in range(n_chip - 1, 0, -1):
            pl.semaphore_signal(barrier, inc=1, device_id=(hub_of[d], my_kv), device_id_type=MESH)
            pl.semaphore_signal(barrier, inc=1, device_id=(leaf_of[d], my_kv), device_id_type=MESH)
        for d in range(n_kv - 1, -1, -1):
            pl.semaphore_signal(barrier, inc=1, device_id=(leaf_of[0], kv_peers[d]), device_id_type=MESH)

    small = [
        pltpu.make_async_copy(src, dst, small_sem.at[i])
        for i, (src, dst) in enumerate(
            ((owner_hbm, owner_ref), (q_hbm, q_ref), (number_hbm, number_ref), (length_hbm, length_ref))
        )
    ]
    for copy in small:
        copy.start()
    for s in range(slots):
        pltpu.make_async_copy(key_hbm.at[s], keys.at[s], page_sem.at[0]).start()
        pltpu.make_async_copy(value_hbm.at[s], values.at[s], page_sem.at[1]).start()

    def remote(src, dst, send, recv, target):
        return pltpu.make_async_remote_copy(
            src_ref=src, dst_ref=dst, send_sem=send, recv_sem=recv,
            device_id=target, device_id_type=MESH,
        )

    def arrived(buffer, count, sem):
        if count:
            pltpu.make_async_copy(buffer.at[pl.ds(0, count)], buffer.at[pl.ds(0, count)], sem).wait()

    small[0].wait()
    lane1 = lax.broadcasted_iota(jnp.int32, (1, HEAD_SIZE), 1)
    own_table = jnp.full((1, HEAD_SIZE), -1.0, jnp.float32)
    for s in range(slots):
        own_table = jnp.where(lane1 == s, owner_ref[s].astype(jnp.float32), own_table)
    table[my_req] = own_table
    small[1].wait()
    for h in range(HQ):
        q_rows[h : h + 1, :] = q_ref[0:1, h * HEAD_SIZE : (h + 1) * HEAD_SIZE].astype(jnp.float32)
    own_query = q_rows[...].astype(jnp.bfloat16)
    q_own[...] = own_query
    small[2].wait()
    small[3].wait()

    pl.semaphore_wait(barrier, n_kv + n_chip - 1 - core)

    mine = core * n_kv + my_kv
    for d in range(n_chip - 1, 0, -1):
        remote(table.at[my_req], table.at[my_req], ts_sem.at[0], tr_sem.at[0], (hub_of[d], my_kv)).start()
    for d in range(n_kv - 1, 0, -1):
        remote(q_own, q_col.at[mine], qs_sem.at[0], qr_sem.at[0], (hub_of[0], kv_peers[d])).start()

    @pl.when(is_leaf)
    def _():
        remote(table.at[my_req], table.at[my_req], ts_sem.at[0], tr_sem.at[0], (hub_of[0], my_kv)).start()
        remote(q_own, q_col.at[mine], qs_sem.at[0], qr_sem.at[0], (hub_of[0], my_kv)).start()

    homes = []
    for d in range(n_chip):
        pair = []
        for b in range(CORES):
            index, present = jnp.int32(0), jnp.int32(0)
            for s in range(slots):
                same = lax.div(owner_ref[s], group) == leaf_of[d] + b
                index = jnp.where(same, jnp.int32(s), index)
                present = jnp.where(same, jnp.int32(1), present)
            limit = length_ref[owner_ref[index]] - number_ref[index] * page_tokens
            pair.append((index, limit * present))
        homes.append(pair)

    edges = [0, max(n_chip // 4, 1), max(3 * n_chip // 4, 1), n_chip]
    stage_of = [sum(d >= edge for edge in edges[1:]) for d in range(n_chip)]

    @pl.when(is_hub)
    def _():
        q_col[(CORES - 1) * n_kv + my_kv] = q_own[...]
        arrived(table, n_req - 1, tr_sem.at[0])
        picks = {}
        for d in range(n_chip - 1, -1, -1):
            for a in range(CORES):
                row = table[leaf_of[d] + a]
                for b in range(CORES):
                    rel = row - ((leaf_of[0] + b) * group).astype(jnp.float32)
                    inside = jnp.logical_and(rel >= 0.0, rel < float(group))
                    picks[d, a, b] = jnp.max(jnp.where(inside, rel, -1.0), axis=1, keepdims=True)
        for (d, a, b), pick in picks.items():
            held[b, d * CORES + a] = jnp.broadcast_to(pick, (1, HEAD_SIZE))
        arrived(q_col, CORES * n_kv - 1, qr_sem.at[0])
        choices = [q_col[c].astype(jnp.float32) for c in range(CORES * group)]
        for d in range(n_chip - 1, -1, -1):
            for a in range(CORES):
                for b in range(CORES):
                    pick = jnp.broadcast_to(picks[d, a, b], (HQ, HEAD_SIZE))
                    chosen = jnp.zeros((HQ, HEAD_SIZE), jnp.float32)
                    for c in range(group):
                        chosen = jnp.where(pick == float(c), choices[b * group + c], chosen)
                    if d == 0 and a == CORES - 1:
                        q_in[my_chip, b] = chosen.astype(jnp.bfloat16)
                    else:
                        q_send[d * CORES + a, b] = chosen.astype(jnp.bfloat16)
                if d or a < CORES - 1:
                    remote(
                        q_send.at[d * CORES + a], q_in.at[my_chip], ds_sem.at[0], dr_sem.at[stage_of[d]],
                        (leaf_of[d] + a, my_kv),
                    ).start()

    pltpu.make_async_copy(key_hbm, keys, page_sem.at[0]).wait()
    pltpu.make_async_copy(value_hbm, values, page_sem.at[1]).wait()

    row = lax.broadcasted_iota(jnp.int32, (HQ, HEAD_SIZE), 0)
    lane = lax.broadcasted_iota(jnp.int32, (HQ, HEAD_SIZE), 1)
    on_diagonal = row == lane
    first = lax.broadcasted_iota(jnp.int32, (PAIR, HEAD_SIZE), 0) < QUERY_PER_KV
    token = lax.broadcasted_iota(jnp.int32, (HQ, page_tokens), 1)
    wide = 2 * HEAD_SIZE

    for stage, (low, high) in enumerate(zip(edges[:-1], edges[1:])):
        batch = [(d, b) for d in range(high - 1, low - 1, -1) for b in range(CORES)]
        if low == 0:

            @pl.when(is_leaf)
            def _():
                arrived(q_in, 1, dr_sem.at[0])

        arrived(q_in, high - max(low, 1), dr_sem.at[stage])
        scored = {}
        for d, b in batch:
            index, limit = homes[d][b]
            query = q_in[chip_peers[d], b].astype(jnp.float32)
            pieces = []
            for k in range(HQ // PAIR):
                q8 = query[k * PAIR : (k + 1) * PAIR]
                both = jnp.concatenate(
                    [jnp.where(first, q8, 0.0), jnp.where(first, 0.0, q8)], axis=1
                ).astype(jnp.bfloat16)
                pieces.append(
                    lax.dot_general(
                        both, keys[index, :, k * wide : (k + 1) * wide],
                        (((1,), (1,)), ((), ())), preferred_element_type=jnp.float32,
                    )
                )
            scores = jnp.concatenate(pieces, axis=0) * HEAD_SIZE ** (-0.5)
            scored[d, b] = jnp.where(token < limit, scores, lowest)
        tops = {e: jnp.max(scored[e], axis=1, keepdims=True) for e in batch}
        weights = {e: jnp.exp(scored[e] - tops[e]) for e in batch}
        totals = {e: jnp.sum(weights[e], axis=1, keepdims=True) for e in batch}
        for d, b in batch:
            index, limit = homes[d][b]
            blocks = []
            for k in range(HQ // PAIR):
                w8 = weights[d, b][k * PAIR : (k + 1) * PAIR].astype(jnp.bfloat16)
                both = jnp.dot(
                    w8, values[index, :, k * wide : (k + 1) * wide], preferred_element_type=jnp.float32
                )
                blocks.append(jnp.where(first, both[:, :HEAD_SIZE], both[:, HEAD_SIZE:]))
            blocks.append(diagonal_to_lanes(tops[d, b], on_diagonal))
            blocks.append(diagonal_to_lanes(totals[d, b], on_diagonal))
            part_send[d, b] = jnp.concatenate(blocks, axis=0)
            if b < CORES - 1:
                continue
            copy = remote(part_send.at[d], part_in.at[my_req], ps_sem.at[0], pr_sem.at[0], (hub_of[d], my_kv))
            if d == 0:
                pl.when(is_leaf)(copy.start)
            else:
                copy.start()

    @pl.when(is_hub)
    def _():
        arrived(part_in, n_req - 1, pr_sem.at[0])
        for b in range(CORES):
            sources = []
            for d in range(n_chip):
                for a in range(CORES):
                    if d == 0 and a == CORES - 1:
                        sources.append(part_send.at[0, b])
                    else:
                        sources.append(part_in.at[leaf_of[d] + a, b])
            tops = [source[HQ : HQ + 1, :] for source in sources]
            totals = [source[HQ + 1 : HQ + 2, :] for source in sources]
            picks = [held[b, e] for e in range(n_req)]
            member = [[picks[e] == float(c) for e in range(n_req)] for c in range(group)]
            merged_top, merged_total = [], []
            for c in range(group):
                best = jnp.full((1, HEAD_SIZE), lowest, jnp.float32)
                for e in range(n_req):
                    best = jnp.maximum(best, jnp.where(member[c][e], tops[e], lowest))
                merged_top.append(best)
            factors = []
            for e in range(n_req):
                best = tops[e]
                for c in range(group):
                    best = jnp.where(member[c][e], merged_top[c], best)
                factors.append(jnp.exp(tops[e] - best))
            for c in range(group):
                amount = jnp.zeros((1, HEAD_SIZE), jnp.float32)
                for e in range(n_req):
                    amount = amount + jnp.where(member[c][e], factors[e] * totals[e], 0.0)
                merged_total.append(amount)
            sums = [jnp.zeros((HQ, HEAD_SIZE), jnp.float32) for _ in range(group)]
            for e in range(n_req):
                scaled = lanes_to_column(factors[e], on_diagonal) * sources[e][0:HQ, :]
                pick = jnp.broadcast_to(picks[e], (HQ, HEAD_SIZE))
                for c in range(group):
                    sums[c] = sums[c] + jnp.where(pick == float(c), scaled, 0.0)
            for c in range(group):
                merged[b * n_kv + c, 0:HQ, :] = sums[c]
                merged[b * n_kv + c, HQ : HQ + 2, :] = jnp.concatenate([merged_top[c], merged_total[c]], axis=0)
            for d in range(n_kv - 1, -1, -1):
                if d == 0 and b == CORES - 1:
                    merged_in[my_kv] = merged[b * n_kv + my_kv]
                    continue
                remote(
                    merged.at[b * n_kv + kv_peers[d]], merged_in.at[my_kv], ms_sem.at[0], mr_sem.at[0],
                    (leaf_of[0] + b, kv_peers[d]),
                ).start()

    @pl.when(is_leaf)
    def _():
        arrived(merged_in, n_kv, mr_sem.at[0])

    @pl.when(is_hub)
    def _():
        arrived(merged_in, n_kv - 1, mr_sem.at[0])

    tops = [merged_in[c, HQ : HQ + 1, :] for c in range(n_kv)]
    best = tops[0]
    for c in range(1, n_kv):
        best = jnp.maximum(best, tops[c])
    factors = [jnp.exp(tops[c] - best) for c in range(n_kv)]
    amount = jnp.zeros((1, HEAD_SIZE), jnp.float32)
    for c in range(n_kv):
        amount = amount + factors[c] * merged_in[c, HQ + 1 : HQ + 2, :]
    result = jnp.zeros((HQ, HEAD_SIZE), jnp.float32)
    for c in range(n_kv):
        result = result + lanes_to_column(factors[c], on_diagonal) * merged_in[c, 0:HQ, :]
    result = result / lanes_to_column(amount, on_diagonal)
    out_ref[...] = result.astype(jnp.bfloat16)

    @pl.when(is_leaf)
    def _():
        arrived(q_col, n_kv, qs_sem.at[0])
        arrived(table, n_chip, ts_sem.at[0])
        arrived(part_send, n_chip, ps_sem.at[0])

    @pl.when(is_hub)
    def _():
        arrived(q_col, n_kv - 1, qs_sem.at[0])
        arrived(table, n_chip - 1, ts_sem.at[0])
        arrived(part_send, n_chip - 1, ps_sem.at[0])
        arrived(q_send, n_req - 1, ds_sem.at[0])
        arrived(merged, CORES * n_kv - 1, ms_sem.at[0])


def solution(mesh):
    n_req, n_kv = mesh.shape["req"], mesh.shape["kv"]

    def on_device(queries, key_cache, value_cache, page_request, page_number, lengths):
        slots, page_tokens, width = key_cache.shape
        group = lengths.shape[0] // n_req
        n_chip = n_req // CORES
        dma = pltpu.SemaphoreType.DMA
        vmem = pl.BlockSpec(memory_space=pltpu.VMEM)
        anywhere = pl.BlockSpec(memory_space=pl.ANY)
        blob = (HQ + 2, HEAD_SIZE)
        attended = pl.pallas_call(
            functools.partial(kernel, n_req, n_kv, group),
            out_shape=pltpu.VMEM((HQ, HEAD_SIZE), jnp.bfloat16),
            in_specs=[anywhere] * 6,
            out_specs=vmem,
            scratch_shapes=[
                pltpu.SMEM(page_request.shape, jnp.int32),
                pltpu.SMEM(page_number.shape, jnp.int32),
                pltpu.SMEM(lengths.shape, jnp.int32),
                pltpu.VMEM(queries.shape, queries.dtype),
                pltpu.VMEM((slots, page_tokens, width), jnp.bfloat16),
                pltpu.VMEM((slots, page_tokens, width), jnp.bfloat16),
                pltpu.VMEM((HQ, HEAD_SIZE), jnp.float32),
                pltpu.VMEM((HQ, HEAD_SIZE), jnp.bfloat16),
                pltpu.VMEM((CORES * n_kv, HQ, HEAD_SIZE), jnp.bfloat16),
                pltpu.VMEM((n_req, 1, HEAD_SIZE), jnp.float32),
                pltpu.VMEM((CORES, n_req, 1, HEAD_SIZE), jnp.float32),
                pltpu.VMEM((n_req, CORES, HQ, HEAD_SIZE), jnp.bfloat16),
                pltpu.VMEM((n_chip, CORES, HQ, HEAD_SIZE), jnp.bfloat16),
                pltpu.VMEM((n_chip, CORES) + blob, jnp.float32),
                pltpu.VMEM((n_req, CORES) + blob, jnp.float32),
                pltpu.VMEM((CORES * n_kv,) + blob, jnp.float32),
                pltpu.VMEM((n_kv,) + blob, jnp.float32),
                dma((4,)),
                dma((2,)),
                dma((1,)), dma((1,)),
                dma((1,)), dma((1,)),
                dma((1,)), dma((3,)),
                dma((1,)), dma((1,)),
                dma((1,)), dma((1,)),
            ],
            compiler_params=pltpu.CompilerParams(collective_id=0, has_side_effects=True),
        )(page_request, page_number, lengths, queries, key_cache, value_cache)
        return attended.reshape(queries.shape)

    placed = (
        P(("req", "kv"), None),
        P(("req", "kv"), None, None),
        P(("req", "kv"), None, None),
        P(("req", "kv")),
        P(("req", "kv")),
        P(),
    )
    return jax.shard_map(
        on_device, mesh=mesh, in_specs=placed, out_specs=P(("req", "kv"), None), check_vma=False
    )
```

```python
import functools

import jax
import jax.numpy as jnp
from jax import lax
from jax.experimental import pallas as pl
from jax.experimental.pallas import tpu as pltpu
from jax.sharding import PartitionSpec as P

HQ = 32
KEY_VALUE_HEADS = 8
HEAD_SIZE = 128
QUERY_PER_KV = 4
CORES = 2
PAIR = 2 * QUERY_PER_KV

lowest = -1e30
finest = 1e-30
STEPS = 32767.0
MESH = pl.DeviceIdType.MESH


def partners(me, n):
    if n & (n - 1):
        return [lax.rem(me + d, n) for d in range(n)]
    found = []
    for d in range(n):
        place, bit = me, 1
        while bit < n:
            if d & bit:
                place = place + bit - 2 * bit * lax.rem(lax.div(me, bit), 2)
            bit *= 2
        found.append(place)
    return found


def diagonal_to_lanes(column, on_diagonal):
    return jnp.sum(jnp.where(on_diagonal, column, 0.0), axis=0, keepdims=True)


def lanes_to_column(row, on_diagonal):
    return jnp.sum(jnp.where(on_diagonal, row, 0.0), axis=1, keepdims=True)


def kernel(
    n_req, n_kv, group,
    owner_hbm, number_hbm, length_hbm, q_hbm, key_hbm, value_hbm, out_ref,
    owner_ref, number_ref, length_ref, q_ref, keys, values, q_rows, q_own, q_col, table, held, q_send, q_in,
    part_send, part_in, stat_send, stat_in, near_send, near_in, near_stat, merged, merged_in,
    met_sem, small_sem, page_sem, qs_sem, qr_sem, ts_sem, tr_sem, ds_sem, dr_sem, ps_sem, pr_sem, ss_sem, sr_sem, ns_sem, nr_sem, ms_sem, mr_sem,
):
    slots, page_tokens, _ = keys.shape
    n_chip = n_req // CORES
    n_near = n_chip
    my_req = lax.axis_index("req")
    my_kv = lax.axis_index("kv")
    my_chip = lax.div(my_req, CORES)
    core = lax.rem(my_req, CORES)
    is_hub = core == CORES - 1
    is_leaf = core < CORES - 1
    is_last = my_kv == n_kv - 1
    is_near = jnp.logical_and(my_kv == 0, my_chip < n_near)
    chip_peers = partners(my_chip, n_chip)
    kv_peers = partners(my_kv, n_kv)
    hub_of = [CORES * chip + CORES - 1 for chip in chip_peers]
    leaf_of = [CORES * chip for chip in chip_peers]

    small = [
        pltpu.make_async_copy(src, dst, small_sem.at[i])
        for i, (src, dst) in enumerate(
            ((owner_hbm, owner_ref), (q_hbm, q_ref), (number_hbm, number_ref), (length_hbm, length_ref))
        )
    ]
    for copy in small[:2]:
        copy.start()

    barrier = pltpu.get_barrier_semaphore()

    @pl.when(is_hub)
    def _():
        for d in range(n_kv - 1, -1, -1):
            pl.semaphore_signal(barrier, inc=1, device_id=(leaf_of[0], kv_peers[d]), device_id_type=MESH)
        for d in range(n_chip - 1, 0, -1):
            pl.semaphore_signal(barrier, inc=1, device_id=(hub_of[d], my_kv), device_id_type=MESH)

    @pl.when(is_leaf)
    def _():
        pl.semaphore_signal(barrier, inc=1, device_id=(hub_of[0], my_kv), device_id_type=MESH)

    def remote(src, dst, send, recv, target):
        return pltpu.make_async_remote_copy(
            src_ref=src, dst_ref=dst, send_sem=send, recv_sem=recv,
            device_id=target, device_id_type=MESH,
        )

    def arrived(buffer, count, sem):
        if count:
            pltpu.make_async_copy(buffer.at[pl.ds(0, count)], buffer.at[pl.ds(0, count)], sem).wait()

    small[1].wait()
    for h in range(HQ):
        q_rows[h : h + 1, :] = q_ref[0:1, h * HEAD_SIZE : (h + 1) * HEAD_SIZE].astype(jnp.float32)
    q_own[...] = q_rows[...].astype(jnp.bfloat16)
    small[0].wait()
    lane1 = lax.broadcasted_iota(jnp.int32, (1, HEAD_SIZE), 1)
    own_table = jnp.full((1, HEAD_SIZE), -1.0, jnp.float32)
    for s in range(slots):
        own_table = jnp.where(lane1 == s, owner_ref[s].astype(jnp.float32), own_table)
    table[my_req] = own_table

    mine = core * n_kv + my_kv

    def send_query():
        for d in range(n_kv - 1, 0, -1):
            remote(q_own, q_col.at[mine], qs_sem.at[0], qr_sem.at[0], (hub_of[0], kv_peers[d])).start()

    def send_table():
        for d in range(n_chip - 1, 0, -1):
            remote(table.at[my_req], table.at[my_req], ts_sem.at[0], tr_sem.at[d], (hub_of[d], my_kv)).start()

    @pl.when(is_leaf)
    def _():
        pl.semaphore_wait(barrier, n_kv)
        pl.semaphore_signal(met_sem, inc=1, device_id=(hub_of[0], my_kv), device_id_type=MESH)
        send_query()
        remote(q_own, q_col.at[mine], qs_sem.at[0], qr_sem.at[0], (hub_of[0], my_kv)).start()
        remote(table.at[my_req], table.at[my_req], ts_sem.at[0], tr_sem.at[0], (hub_of[0], my_kv)).start()
        pl.semaphore_wait(met_sem, 1)
        send_table()

    @pl.when(is_hub)
    def _():
        pl.semaphore_wait(barrier, n_chip)
        pl.semaphore_signal(met_sem, inc=1, device_id=(leaf_of[0], my_kv), device_id_type=MESH)
        send_table()
        pl.semaphore_wait(met_sem, 1)
        send_query()

    for copy in small[2:]:
        copy.start()
    for s in range(slots):
        pltpu.make_async_copy(key_hbm.at[s], keys.at[s], page_sem.at[0]).start()
        pltpu.make_async_copy(value_hbm.at[s], values.at[s], page_sem.at[1]).start()
    for copy in small[2:]:
        copy.wait()

    homes = []
    for d in range(n_chip):
        pair = []
        for b in range(CORES):
            index, present = jnp.int32(0), jnp.int32(0)
            for s in range(slots):
                same = lax.div(owner_ref[s], group) == d * CORES + b
                index = jnp.where(same, jnp.int32(s), index)
                present = jnp.where(same, jnp.int32(1), present)
            limit = length_ref[owner_ref[index]] - number_ref[index] * page_tokens
            place = jnp.where(present == 1, owner_ref[index] - (d * CORES + b) * group, -1)
            pair.append((index, limit * present, place))
        homes.append(pair)

    edges = [0, max(n_chip // 4, 1), max(3 * n_chip // 4, 1), n_chip]
    alone = [jnp.logical_and(is_hub, my_chip == c) for c in range(n_chip)]
    met = [jnp.logical_not(own) for own in alone]

    @pl.when(is_hub)
    def _():
        q_col[(CORES - 1) * n_kv + my_kv] = q_own[...]
        arrived(q_col, CORES * n_kv - 1, qr_sem.at[0])
        choices = [q_col[c].astype(jnp.float32) for c in range(CORES * group)]
        for d in range(n_chip):
            arrived(table, CORES if d else CORES - 1, tr_sem.at[d])
            picks = {}
            for a in range(CORES):
                row = table[leaf_of[d] + a]
                for b in range(CORES):
                    rel = row - ((leaf_of[0] + b) * group).astype(jnp.float32)
                    inside = jnp.logical_and(rel >= 0.0, rel < float(group))
                    picks[a, b] = jnp.max(jnp.where(inside, rel, -1.0), axis=1, keepdims=True)
            for a in range(CORES):
                for b in range(CORES):
                    held[b, leaf_of[d] + a] = jnp.broadcast_to(picks[a, b], (1, HEAD_SIZE))
                    pick = jnp.broadcast_to(picks[a, b], (HQ, HEAD_SIZE))
                    chosen = jnp.zeros((HQ, HEAD_SIZE), jnp.float32)
                    for c in range(group):
                        chosen = jnp.where(pick == float(c), choices[b * group + c], chosen)
                    if d == 0 and a == CORES - 1:
                        q_in[my_chip, b] = chosen.astype(jnp.bfloat16)
                    else:
                        q_send[d * CORES + a, b] = chosen.astype(jnp.bfloat16)
                if d or a < CORES - 1:
                    remote(
                        q_send.at[d * CORES + a], q_in.at[my_chip], ds_sem.at[0], dr_sem.at[my_chip],
                        (leaf_of[d] + a, my_kv),
                    ).start()

    pltpu.make_async_copy(key_hbm, keys, page_sem.at[0]).wait()
    pltpu.make_async_copy(value_hbm, values, page_sem.at[1]).wait()

    row = lax.broadcasted_iota(jnp.int32, (HQ, HEAD_SIZE), 0)
    lane = lax.broadcasted_iota(jnp.int32, (HQ, HEAD_SIZE), 1)
    on_diagonal = row == lane
    first = lax.broadcasted_iota(jnp.int32, (PAIR, HEAD_SIZE), 0) < QUERY_PER_KV
    token = lax.broadcasted_iota(jnp.int32, (HQ, page_tokens), 1)
    wide = 2 * HEAD_SIZE

    for stage, (low, high) in enumerate(zip(edges[:-1], edges[1:])):
        batch = [(c, b) for c in range(low, high) for b in range(CORES)]
        for c in range(low, high):

            @pl.when(met[c])
            def _():
                arrived(q_in, 1, dr_sem.at[c])

        scored = {}
        for d, b in batch:
            index, limit, _ = homes[d][b]
            query = q_in[d, b].astype(jnp.float32)
            pieces = []
            for k in range(HQ // PAIR):
                q8 = query[k * PAIR : (k + 1) * PAIR]
                both = jnp.concatenate(
                    [jnp.where(first, q8, 0.0), jnp.where(first, 0.0, q8)], axis=1
                ).astype(jnp.bfloat16)
                pieces.append(
                    lax.dot_general(
                        both, keys[index, :, k * wide : (k + 1) * wide],
                        (((1,), (1,)), ((), ())), preferred_element_type=jnp.float32,
                    )
                )
            scores = jnp.concatenate(pieces, axis=0) * HEAD_SIZE ** (-0.5)
            scored[d, b] = jnp.where(token < limit, scores, lowest)
        tops = {e: jnp.max(scored[e], axis=1, keepdims=True) for e in batch}
        weights = {e: jnp.exp(scored[e] - tops[e]) for e in batch}
        totals = {e: jnp.sum(weights[e], axis=1, keepdims=True) for e in batch}
        summed, largest = {}, {}
        for d, b in batch:
            index, _, _ = homes[d][b]
            blocks = []
            for k in range(HQ // PAIR):
                w8 = weights[d, b][k * PAIR : (k + 1) * PAIR].astype(jnp.bfloat16)
                both = jnp.dot(
                    w8, values[index, :, k * wide : (k + 1) * wide], preferred_element_type=jnp.float32
                )
                blocks.append(jnp.where(first, both[:, :HEAD_SIZE], both[:, HEAD_SIZE:]))
            blocks = jnp.concatenate(blocks, axis=0)
            largest[d, b] = jnp.maximum(jnp.max(jnp.abs(blocks), axis=1, keepdims=True), finest)
            summed[d, b] = blocks
        for d, b in batch:
            coded = jnp.round(summed[d, b] * (STEPS / largest[d, b]))
            part_send[d, b] = coded.astype(jnp.int32).astype(jnp.int16)
            lanes = [diagonal_to_lanes(column[d, b], on_diagonal) for column in (tops, totals, largest)]
            stat_send[d, b] = jnp.concatenate(lanes, axis=0)
            if d < n_near:
                lanes[0] = jnp.where(homes[d][b][2] == 0, lanes[0], lowest)
                near_send[d, b] = jnp.concatenate(lanes, axis=0)
            if b < CORES - 1:
                continue
            target = (d * CORES + CORES - 1, my_kv)
            copy = remote(part_send.at[d], part_in.at[my_req], ps_sem.at[0], pr_sem.at[0], target)
            stat_copy = remote(stat_send.at[d], stat_in.at[my_req], ss_sem.at[0], sr_sem.at[0], target)

            if d < n_near:

                @pl.when(is_last)
                def _():
                    for a in range(CORES):
                        owner = (d * CORES + a, 0)
                        remote(near_send.at[d, a], near_stat.at[my_req], ns_sem.at[0], nr_sem.at[0], owner).start()
                        remote(part_send.at[d, a], near_in.at[my_req], ns_sem.at[1], nr_sem.at[1], owner).start()

            @pl.when(met[d])
            def _():
                stat_copy.start()
                copy.start()


    @pl.when(is_hub)
    def _():
        part_in[my_req] = part_send[my_chip]
        stat_in[my_req] = stat_send[my_chip]
        arrived(stat_in, n_req - 1, sr_sem.at[0])
        arrived(part_in, n_req - 1, pr_sem.at[0])
        for b in range(CORES):
            sources = [part_in.at[e, b] for e in range(n_req)]
            stats = [stat_in.at[e, b] for e in range(n_req)]
            tops = [stat[0:1, :] for stat in stats]
            totals = [stat[1:2, :] for stat in stats]
            steps = [stat[2:3, :] * (1.0 / STEPS) for stat in stats]
            picks = [held[b, e] for e in range(n_req)]
            member = [[picks[e] == float(c) for e in range(n_req)] for c in range(group)]
            merged_top, merged_total = [], []
            for c in range(group):
                best = jnp.full((1, HEAD_SIZE), lowest, jnp.float32)
                for e in range(n_req):
                    best = jnp.maximum(best, jnp.where(member[c][e], tops[e], lowest))
                merged_top.append(best)
            factors = []
            for e in range(n_req):
                best = tops[e]
                for c in range(group):
                    best = jnp.where(member[c][e], merged_top[c], best)
                factors.append(jnp.exp(tops[e] - best))
            for c in range(group):
                amount = jnp.zeros((1, HEAD_SIZE), jnp.float32)
                for e in range(n_req):
                    amount = amount + jnp.where(member[c][e], factors[e] * totals[e], 0.0)
                merged_total.append(amount)
            sums = [jnp.zeros((HQ, HEAD_SIZE), jnp.float32) for _ in range(group)]
            for e in range(n_req):
                coded = sources[e][...].astype(jnp.int32).astype(jnp.float32)
                scaled = lanes_to_column(factors[e] * steps[e], on_diagonal) * coded
                pick = jnp.broadcast_to(picks[e], (HQ, HEAD_SIZE))
                for c in range(group):
                    sums[c] = sums[c] + jnp.where(pick == float(c), scaled, 0.0)
            for c in range(group):
                merged[b * n_kv + c, 0:HQ, :] = sums[c]
                merged[b * n_kv + c, HQ : HQ + 2, :] = jnp.concatenate([merged_top[c], merged_total[c]], axis=0)
            for d in range(n_kv - 1, -1, -1):
                if d == 0 and b == CORES - 1:
                    merged_in[my_kv] = merged[b * n_kv + my_kv]
                    continue
                copy = remote(
                    merged.at[b * n_kv + kv_peers[d]], merged_in.at[my_kv], ms_sem.at[0], mr_sem.at[0],
                    (leaf_of[0] + b, kv_peers[d]),
                )
                if d == 0:
                    copy.start()
                else:
                    skipped = jnp.logical_and(jnp.logical_and(is_last, kv_peers[d] == 0), my_chip < n_near)
                    pl.when(jnp.logical_not(skipped))(copy.start)

    for role, others in ((is_leaf, n_kv), (is_hub, n_kv - 1)):

        @pl.when(jnp.logical_and(role, jnp.logical_not(is_near)))
        def _():
            arrived(merged_in, others, mr_sem.at[0])

        @pl.when(jnp.logical_and(role, is_near))
        def _():
            arrived(merged_in, others - 1, mr_sem.at[0])

    @pl.when(is_near)
    def _():
        arrived(near_stat, n_req, nr_sem.at[0])
        tops = [near_stat[e, 0:1, :] for e in range(n_req)]
        best = tops[0]
        for e in range(1, n_req):
            best = jnp.maximum(best, tops[e])
        factors = [jnp.exp(tops[e] - best) for e in range(n_req)]
        amount = jnp.zeros((1, HEAD_SIZE), jnp.float32)
        for e in range(n_req):
            amount = amount + factors[e] * near_stat[e, 1:2, :]
        arrived(near_in, n_req, nr_sem.at[1])
        total = jnp.zeros((HQ, HEAD_SIZE), jnp.float32)
        for e in range(n_req):
            step = factors[e] * (near_stat[e, 2:3, :] * (1.0 / STEPS))
            total = total + lanes_to_column(step, on_diagonal) * near_in[e].astype(jnp.int32).astype(jnp.float32)
        merged_in[n_kv - 1, 0:HQ, :] = total
        merged_in[n_kv - 1, HQ : HQ + 2, :] = jnp.concatenate([best, amount], axis=0)

    tops = [merged_in[c, HQ : HQ + 1, :] for c in range(n_kv)]
    best = tops[0]
    for c in range(1, n_kv):
        best = jnp.maximum(best, tops[c])
    factors = [jnp.exp(tops[c] - best) for c in range(n_kv)]
    amount = jnp.zeros((1, HEAD_SIZE), jnp.float32)
    for c in range(n_kv):
        amount = amount + factors[c] * merged_in[c, HQ + 1 : HQ + 2, :]
    result = jnp.zeros((HQ, HEAD_SIZE), jnp.float32)
    for c in range(n_kv):
        result = result + lanes_to_column(factors[c], on_diagonal) * merged_in[c, 0:HQ, :]
    result = result / lanes_to_column(amount, on_diagonal)
    out_ref[...] = result.astype(jnp.bfloat16)

    @pl.when(is_leaf)
    def _():
        arrived(q_col, n_kv, qs_sem.at[0])
        arrived(table, n_chip, ts_sem.at[0])
        arrived(part_send, n_chip, ps_sem.at[0])
        arrived(stat_send, n_chip, ss_sem.at[0])

    @pl.when(is_hub)
    def _():
        arrived(q_col, n_kv - 1, qs_sem.at[0])
        arrived(table, n_chip - 1, ts_sem.at[0])
        arrived(part_send, n_chip - 1, ps_sem.at[0])
        arrived(stat_send, n_chip - 1, ss_sem.at[0])
        arrived(q_send, n_req - 1, ds_sem.at[0])

    sends_near = jnp.logical_and(is_last, my_chip < n_near)

    @pl.when(jnp.logical_and(is_hub, jnp.logical_not(sends_near)))
    def _():
        arrived(merged, CORES * n_kv - 1, ms_sem.at[0])

    @pl.when(jnp.logical_and(is_hub, sends_near))
    def _():
        arrived(merged, CORES * n_kv - 1 - CORES, ms_sem.at[0])

    @pl.when(is_last)
    def _():
        arrived(near_send, n_near, ns_sem.at[0])
        arrived(part_send, n_near, ns_sem.at[1])


def solution(mesh):
    n_req, n_kv = mesh.shape["req"], mesh.shape["kv"]

    def on_device(queries, key_cache, value_cache, page_request, page_number, lengths):
        slots, page_tokens, width = key_cache.shape
        group = lengths.shape[0] // n_req
        n_chip = n_req // CORES
        dma = pltpu.SemaphoreType.DMA
        vmem = pl.BlockSpec(memory_space=pltpu.VMEM)
        anywhere = pl.BlockSpec(memory_space=pl.ANY)
        blob = (HQ + 2, HEAD_SIZE)
        attended = pl.pallas_call(
            functools.partial(kernel, n_req, n_kv, group),
            out_shape=pltpu.VMEM((HQ, HEAD_SIZE), jnp.bfloat16),
            in_specs=[anywhere] * 6,
            out_specs=vmem,
            scratch_shapes=[
                pltpu.SMEM(page_request.shape, jnp.int32),
                pltpu.SMEM(page_number.shape, jnp.int32),
                pltpu.SMEM(lengths.shape, jnp.int32),
                pltpu.VMEM(queries.shape, queries.dtype),
                pltpu.VMEM((slots, page_tokens, width), jnp.bfloat16),
                pltpu.VMEM((slots, page_tokens, width), jnp.bfloat16),
                pltpu.VMEM((HQ, HEAD_SIZE), jnp.float32),
                pltpu.VMEM((HQ, HEAD_SIZE), jnp.bfloat16),
                pltpu.VMEM((CORES * n_kv, HQ, HEAD_SIZE), jnp.bfloat16),
                pltpu.VMEM((n_req, 1, HEAD_SIZE), jnp.float32),
                pltpu.VMEM((CORES, n_req, 1, HEAD_SIZE), jnp.float32),
                pltpu.VMEM((n_req, CORES, HQ, HEAD_SIZE), jnp.bfloat16),
                pltpu.VMEM((n_chip, CORES, HQ, HEAD_SIZE), jnp.bfloat16),
                pltpu.VMEM((n_chip, CORES, HQ, HEAD_SIZE), jnp.int16),
                pltpu.VMEM((n_req, CORES, HQ, HEAD_SIZE), jnp.int16),
                pltpu.VMEM((n_chip, CORES, 3, HEAD_SIZE), jnp.float32),
                pltpu.VMEM((n_req, CORES, 3, HEAD_SIZE), jnp.float32),
                pltpu.VMEM((n_chip, CORES, 3, HEAD_SIZE), jnp.float32),
                pltpu.VMEM((n_req, HQ, HEAD_SIZE), jnp.int16),
                pltpu.VMEM((n_req, 3, HEAD_SIZE), jnp.float32),
                pltpu.VMEM((CORES * n_kv,) + blob, jnp.float32),
                pltpu.VMEM((n_kv,) + blob, jnp.float32),
                pltpu.SemaphoreType.REGULAR,
                dma((4,)),
                dma((2,)),
                dma((1,)), dma((1,)),
                dma((1,)), dma((n_chip,)),
                dma((1,)), dma((n_chip,)),
                dma((1,)), dma((1,)),
                dma((1,)), dma((1,)),
                dma((2,)), dma((2,)),
                dma((1,)), dma((1,)),
            ],
            compiler_params=pltpu.CompilerParams(collective_id=0, has_side_effects=True),
        )(page_request, page_number, lengths, queries, key_cache, value_cache)
        return attended.reshape(queries.shape)

    placed = (
        P(("req", "kv"), None),
        P(("req", "kv"), None, None),
        P(("req", "kv"), None, None),
        P(("req", "kv")),
        P(("req", "kv")),
        P(),
    )
    return jax.shard_map(
        on_device, mesh=mesh, in_specs=placed, out_specs=P(("req", "kv"), None), check_vma=False
    )
```

```python
import functools

import jax
import jax.numpy as jnp
from jax import lax
from jax.experimental import pallas as pl
from jax.experimental.pallas import tpu as pltpu
from jax.sharding import PartitionSpec as P

HQ = 32
KEY_VALUE_HEADS = 8
HEAD_SIZE = 128
QUERY_PER_KV = 4
CORES = 2
PAIR = 2 * QUERY_PER_KV

lowest = -1e30
finest = 1e-30
STEPS = 32767.0
MESH = pl.DeviceIdType.MESH


def partners(me, n):
    if n & (n - 1):
        return [lax.rem(me + d, n) for d in range(n)]
    found = []
    for d in range(n):
        place, bit = me, 1
        while bit < n:
            if d & bit:
                place = place + bit - 2 * bit * lax.rem(lax.div(me, bit), 2)
            bit *= 2
        found.append(place)
    return found


def diagonal_to_lanes(column, on_diagonal):
    return jnp.sum(jnp.where(on_diagonal, column, 0.0), axis=0, keepdims=True)


def lanes_to_column(row, on_diagonal):
    return jnp.sum(jnp.where(on_diagonal, row, 0.0), axis=1, keepdims=True)


def kernel(
    n_req, n_kv, group,
    owner_hbm, number_hbm, length_hbm, q_hbm, key_hbm, value_hbm, out_ref,
    owner_ref, number_ref, length_ref, q_ref, keys, values, q_rows, q_own, q_col, table, held, q_send, q_in,
    part_send, part_in, stat_send, stat_in, near_send, near_in, near_stat, merged, merged_in,
    met_sem, far_sem, small_sem, page_sem, qs_sem, qr_sem, ts_sem, tr_sem, ds_sem, dr_sem, ps_sem, pr_sem, ss_sem, sr_sem, ns_sem, nr_sem, ms_sem, mr_sem,
):
    slots, page_tokens, _ = keys.shape
    n_chip = n_req // CORES
    n_near = n_chip
    my_req = lax.axis_index("req")
    my_kv = lax.axis_index("kv")
    my_chip = lax.div(my_req, CORES)
    core = lax.rem(my_req, CORES)
    is_hub = core == CORES - 1
    is_leaf = core < CORES - 1
    is_last = my_kv == n_kv - 1
    is_relay = my_kv == n_kv - 2
    is_early = my_kv < n_kv - 2
    is_near = jnp.logical_and(my_kv == 0, my_chip < n_near)
    chip_peers = partners(my_chip, n_chip)
    kv_peers = partners(my_kv, n_kv)
    hub_of = [CORES * chip + CORES - 1 for chip in chip_peers]
    leaf_of = [CORES * chip for chip in chip_peers]

    small = [
        pltpu.make_async_copy(src, dst, small_sem.at[i])
        for i, (src, dst) in enumerate(
            ((owner_hbm, owner_ref), (q_hbm, q_ref), (number_hbm, number_ref), (length_hbm, length_ref))
        )
    ]
    for copy in small[:2]:
        copy.start()

    barrier = pltpu.get_barrier_semaphore()

    @pl.when(is_hub)
    def _():
        for z in range(n_kv - 1, -1, -1):

            @pl.when(jnp.logical_not(jnp.logical_and(is_last, z < n_kv - 2)))
            def _():
                pl.semaphore_signal(barrier, inc=1, device_id=(leaf_of[0], z), device_id_type=MESH)

        for d in range(n_chip - 1, 0, -1):
            pl.semaphore_signal(barrier, inc=1, device_id=(hub_of[d], my_kv), device_id_type=MESH)

    @pl.when(is_leaf)
    def _():
        pl.semaphore_signal(barrier, inc=1, device_id=(hub_of[0], my_kv), device_id_type=MESH)

    def remote(src, dst, send, recv, target):
        return pltpu.make_async_remote_copy(
            src_ref=src, dst_ref=dst, send_sem=send, recv_sem=recv,
            device_id=target, device_id_type=MESH,
        )

    def arrived(buffer, count, sem):
        if count:
            pltpu.make_async_copy(buffer.at[pl.ds(0, count)], buffer.at[pl.ds(0, count)], sem).wait()

    small[1].wait()
    for h in range(HQ):
        q_rows[h : h + 1, :] = q_ref[0:1, h * HEAD_SIZE : (h + 1) * HEAD_SIZE].astype(jnp.float32)
    q_own[...] = q_rows[...].astype(jnp.bfloat16)
    small[0].wait()
    lane1 = lax.broadcasted_iota(jnp.int32, (1, HEAD_SIZE), 1)
    own_table = jnp.full((1, HEAD_SIZE), -1.0, jnp.float32)
    for s in range(slots):
        own_table = jnp.where(lane1 == s, owner_ref[s].astype(jnp.float32), own_table)
    table[my_req] = own_table

    mine = core * n_kv + my_kv

    def send_query(last):
        for z in range(last, -1, -1):

            @pl.when(my_kv != z)
            def _():
                remote(q_own, q_col.at[mine], qs_sem.at[0], qr_sem.at[0], (hub_of[0], z)).start()

    def send_table():
        for d in range(n_chip - 1, 0, -1):
            remote(table.at[my_req], table.at[my_req], ts_sem.at[0], tr_sem.at[d], (hub_of[d], my_kv)).start()

    def leaf_column(early):
        pl.semaphore_wait(barrier, n_kv - 1 if early else n_kv)
        pl.semaphore_signal(met_sem, inc=1, device_id=(hub_of[0], my_kv), device_id_type=MESH)
        remote(q_own, q_col.at[mine], qs_sem.at[0], qr_sem.at[1], (hub_of[0], my_kv)).start()
        send_query(n_kv - 2 if early else n_kv - 1)

        @pl.when(is_relay)
        def _():
            for z in range(n_kv - 2):
                pl.semaphore_signal(far_sem, inc=1, device_id=(hub_of[0], z), device_id_type=MESH)

    def leaf_plane():
        pl.semaphore_wait(met_sem, 1)
        send_table()
        remote(table.at[my_req], table.at[my_req], ts_sem.at[0], tr_sem.at[0], (hub_of[0], my_kv)).start()

    def hub_column(early):
        pl.semaphore_wait(met_sem, 1)
        send_query(n_kv - 2 if early else n_kv - 1)
        if early:
            arrived(q_col, 1, qr_sem.at[1])
            pl.semaphore_wait(far_sem, 1)
            last = (hub_of[0], n_kv - 1)
            remote(q_own, q_col.at[mine], qs_sem.at[0], qr_sem.at[0], last).start()
            remote(q_col.at[my_kv], q_col.at[my_kv], qs_sem.at[0], qr_sem.at[0], last).start()

    def hub_plane():
        pl.semaphore_wait(barrier, n_chip)
        pl.semaphore_signal(met_sem, inc=1, device_id=(leaf_of[0], my_kv), device_id_type=MESH)
        send_table()

    for role, column, plane in ((is_leaf, leaf_column, leaf_plane), (is_hub, hub_column, hub_plane)):

        @pl.when(jnp.logical_and(role, jnp.logical_not(is_early)))
        def _():
            column(False)
            plane()

        @pl.when(jnp.logical_and(role, is_early))
        def _():
            plane()
            column(True)

    for copy in small[2:]:
        copy.start()
    for s in range(slots):
        pltpu.make_async_copy(key_hbm.at[s], keys.at[s], page_sem.at[0]).start()
        pltpu.make_async_copy(value_hbm.at[s], values.at[s], page_sem.at[1]).start()
    for copy in small[2:]:
        copy.wait()

    homes = []
    for d in range(n_chip):
        pair = []
        for b in range(CORES):
            index, present = jnp.int32(0), jnp.int32(0)
            for s in range(slots):
                same = lax.div(owner_ref[s], group) == d * CORES + b
                index = jnp.where(same, jnp.int32(s), index)
                present = jnp.where(same, jnp.int32(1), present)
            limit = length_ref[owner_ref[index]] - number_ref[index] * page_tokens
            place = jnp.where(present == 1, owner_ref[index] - (d * CORES + b) * group, -1)
            pair.append((index, limit * present, place))
        homes.append(pair)

    edges = [0, max(n_chip // 4, 1), max(3 * n_chip // 4, 1), n_chip]
    alone = [jnp.logical_and(is_hub, my_chip == c) for c in range(n_chip)]
    met = [jnp.logical_not(own) for own in alone]

    @pl.when(is_hub)
    def _():
        q_col[(CORES - 1) * n_kv + my_kv] = q_own[...]
        arrived(q_col, CORES * n_kv - 2, qr_sem.at[0])

        @pl.when(jnp.logical_not(is_early))
        def _():
            arrived(q_col, 1, qr_sem.at[1])

        choices = [q_col[c].astype(jnp.float32) for c in range(CORES * group)]
        for d in range(n_chip - 1, -1, -1):
            arrived(table, CORES if d else CORES - 1, tr_sem.at[d])
            picks = {}
            for a in range(CORES):
                row = table[leaf_of[d] + a]
                for b in range(CORES):
                    rel = row - ((leaf_of[0] + b) * group).astype(jnp.float32)
                    inside = jnp.logical_and(rel >= 0.0, rel < float(group))
                    picks[a, b] = jnp.max(jnp.where(inside, rel, -1.0), axis=1, keepdims=True)
            for a in range(CORES):
                for b in range(CORES):
                    held[b, leaf_of[d] + a] = jnp.broadcast_to(picks[a, b], (1, HEAD_SIZE))
                    pick = jnp.broadcast_to(picks[a, b], (HQ, HEAD_SIZE))
                    chosen = jnp.zeros((HQ, HEAD_SIZE), jnp.float32)
                    for c in range(group):
                        chosen = jnp.where(pick == float(c), choices[b * group + c], chosen)
                    if d == 0 and a == CORES - 1:
                        q_in[my_chip, b] = chosen.astype(jnp.bfloat16)
                    else:
                        q_send[d * CORES + a, b] = chosen.astype(jnp.bfloat16)
                if d or a < CORES - 1:
                    remote(
                        q_send.at[d * CORES + a], q_in.at[my_chip], ds_sem.at[0], dr_sem.at[my_chip],
                        (leaf_of[d] + a, my_kv),
                    ).start()

    pltpu.make_async_copy(key_hbm, keys, page_sem.at[0]).wait()
    pltpu.make_async_copy(value_hbm, values, page_sem.at[1]).wait()

    row = lax.broadcasted_iota(jnp.int32, (HQ, HEAD_SIZE), 0)
    lane = lax.broadcasted_iota(jnp.int32, (HQ, HEAD_SIZE), 1)
    on_diagonal = row == lane
    first = lax.broadcasted_iota(jnp.int32, (PAIR, HEAD_SIZE), 0) < QUERY_PER_KV
    token = lax.broadcasted_iota(jnp.int32, (HQ, page_tokens), 1)
    wide = 2 * HEAD_SIZE

    for stage, (low, high) in enumerate(zip(edges[:-1], edges[1:])):
        batch = [(c, b) for c in range(low, high) for b in range(CORES)]
        for c in range(low, high):

            @pl.when(met[c])
            def _():
                arrived(q_in, 1, dr_sem.at[c])

        scored = {}
        for d, b in batch:
            index, limit, _ = homes[d][b]
            query = q_in[d, b].astype(jnp.float32)
            pieces = []
            for k in range(HQ // PAIR):
                q8 = query[k * PAIR : (k + 1) * PAIR]
                both = jnp.concatenate(
                    [jnp.where(first, q8, 0.0), jnp.where(first, 0.0, q8)], axis=1
                ).astype(jnp.bfloat16)
                pieces.append(
                    lax.dot_general(
                        both, keys[index, :, k * wide : (k + 1) * wide],
                        (((1,), (1,)), ((), ())), preferred_element_type=jnp.float32,
                    )
                )
            scores = jnp.concatenate(pieces, axis=0) * HEAD_SIZE ** (-0.5)
            scored[d, b] = jnp.where(token < limit, scores, lowest)
        tops = {e: jnp.max(scored[e], axis=1, keepdims=True) for e in batch}
        weights = {e: jnp.exp(scored[e] - tops[e]) for e in batch}
        totals = {e: jnp.sum(weights[e], axis=1, keepdims=True) for e in batch}
        summed, largest = {}, {}
        for d, b in batch:
            index, _, _ = homes[d][b]
            blocks = []
            for k in range(HQ // PAIR):
                w8 = weights[d, b][k * PAIR : (k + 1) * PAIR].astype(jnp.bfloat16)
                both = jnp.dot(
                    w8, values[index, :, k * wide : (k + 1) * wide], preferred_element_type=jnp.float32
                )
                blocks.append(jnp.where(first, both[:, :HEAD_SIZE], both[:, HEAD_SIZE:]))
            blocks = jnp.concatenate(blocks, axis=0)
            largest[d, b] = jnp.maximum(jnp.max(jnp.abs(blocks), axis=1, keepdims=True), finest)
            summed[d, b] = blocks
        for d, b in batch:
            coded = jnp.round(summed[d, b] * (STEPS / largest[d, b]))
            part_send[d, b] = coded.astype(jnp.int32).astype(jnp.int16)
            lanes = [diagonal_to_lanes(column[d, b], on_diagonal) for column in (tops, totals, largest)]
            stat_send[d, b] = jnp.concatenate(lanes, axis=0)
            if d < n_near:
                lanes[0] = jnp.where(homes[d][b][2] == 0, lanes[0], lowest)
                near_send[d, b] = jnp.concatenate(lanes, axis=0)
            if b < CORES - 1:
                continue
            target = (d * CORES + CORES - 1, my_kv)
            copy = remote(part_send.at[d], part_in.at[my_req], ps_sem.at[0], pr_sem.at[0], target)
            stat_copy = remote(stat_send.at[d], stat_in.at[my_req], ss_sem.at[0], sr_sem.at[0], target)

            if d < n_near:

                @pl.when(is_last)
                def _():
                    for a in range(CORES):
                        owner = (d * CORES + a, 0)
                        remote(near_send.at[d, a], near_stat.at[my_req], ns_sem.at[0], nr_sem.at[0], owner).start()
                        remote(part_send.at[d, a], near_in.at[my_req], ns_sem.at[1], nr_sem.at[1], owner).start()

            @pl.when(met[d])
            def _():
                stat_copy.start()
                copy.start()


    def send_merged(b, z):
        skipped = is_last if z == 0 and n_near == n_chip else jnp.bool_(False)
        if b == CORES - 1:
            skipped = jnp.logical_or(skipped, my_kv == z)

        @pl.when(jnp.logical_not(skipped))
        def _():
            remote(
                merged.at[b * n_kv + z], merged_in.at[my_kv], ms_sem.at[0], mr_sem.at[0], (leaf_of[0] + b, z)
            ).start()

    @pl.when(is_hub)
    def _():
        part_in[my_req] = part_send[my_chip]
        stat_in[my_req] = stat_send[my_chip]
        arrived(stat_in, n_req - 1, sr_sem.at[0])
        arrived(part_in, n_req - 1, pr_sem.at[0])
        for b in range(CORES):
            sources = [part_in.at[e, b] for e in range(n_req)]
            stats = [stat_in.at[e, b] for e in range(n_req)]
            tops = [stat[0:1, :] for stat in stats]
            totals = [stat[1:2, :] for stat in stats]
            steps = [stat[2:3, :] * (1.0 / STEPS) for stat in stats]
            picks = [held[b, e] for e in range(n_req)]
            member = [[picks[e] == float(c) for e in range(n_req)] for c in range(group)]
            merged_top, merged_total = [], []
            for c in range(group):
                best = jnp.full((1, HEAD_SIZE), lowest, jnp.float32)
                for e in range(n_req):
                    best = jnp.maximum(best, jnp.where(member[c][e], tops[e], lowest))
                merged_top.append(best)
            factors = []
            for e in range(n_req):
                best = tops[e]
                for c in range(group):
                    best = jnp.where(member[c][e], merged_top[c], best)
                factors.append(jnp.exp(tops[e] - best))
            for c in range(group):
                amount = jnp.zeros((1, HEAD_SIZE), jnp.float32)
                for e in range(n_req):
                    amount = amount + jnp.where(member[c][e], factors[e] * totals[e], 0.0)
                merged_total.append(amount)
            sums = [jnp.zeros((HQ, HEAD_SIZE), jnp.float32) for _ in range(group)]
            for e in range(n_req):
                coded = sources[e][...].astype(jnp.int32).astype(jnp.float32)
                scaled = lanes_to_column(factors[e] * steps[e], on_diagonal) * coded
                pick = jnp.broadcast_to(picks[e], (HQ, HEAD_SIZE))
                for c in range(group):
                    sums[c] = sums[c] + jnp.where(pick == float(c), scaled, 0.0)
            for c in range(group):
                merged[b * n_kv + c, 0:HQ, :] = sums[c]
                merged[b * n_kv + c, HQ : HQ + 2, :] = jnp.concatenate([merged_top[c], merged_total[c]], axis=0)
            send_merged(b, 0)

        for z in range(1, n_kv):
            for b in range(CORES):
                send_merged(b, z)
        merged_in[my_kv] = merged[(CORES - 1) * n_kv + my_kv]

    for role, others in ((is_leaf, n_kv), (is_hub, n_kv - 1)):

        @pl.when(jnp.logical_and(role, jnp.logical_not(is_near)))
        def _():
            arrived(merged_in, others, mr_sem.at[0])

        @pl.when(jnp.logical_and(role, is_near))
        def _():
            arrived(merged_in, others - 1, mr_sem.at[0])

    @pl.when(is_near)
    def _():
        arrived(near_stat, n_req, nr_sem.at[0])
        tops = [near_stat[e, 0:1, :] for e in range(n_req)]
        best = tops[0]
        for e in range(1, n_req):
            best = jnp.maximum(best, tops[e])
        factors = [jnp.exp(tops[e] - best) for e in range(n_req)]
        amount = jnp.zeros((1, HEAD_SIZE), jnp.float32)
        for e in range(n_req):
            amount = amount + factors[e] * near_stat[e, 1:2, :]
        arrived(near_in, n_req, nr_sem.at[1])
        total = jnp.zeros((HQ, HEAD_SIZE), jnp.float32)
        for e in range(n_req):
            step = factors[e] * (near_stat[e, 2:3, :] * (1.0 / STEPS))
            total = total + lanes_to_column(step, on_diagonal) * near_in[e].astype(jnp.int32).astype(jnp.float32)
        merged_in[n_kv - 1, 0:HQ, :] = total
        merged_in[n_kv - 1, HQ : HQ + 2, :] = jnp.concatenate([best, amount], axis=0)

    tops = [merged_in[c, HQ : HQ + 1, :] for c in range(n_kv)]
    best = tops[0]
    for c in range(1, n_kv):
        best = jnp.maximum(best, tops[c])
    factors = [jnp.exp(tops[c] - best) for c in range(n_kv)]
    amount = jnp.zeros((1, HEAD_SIZE), jnp.float32)
    for c in range(n_kv):
        amount = amount + factors[c] * merged_in[c, HQ + 1 : HQ + 2, :]
    result = jnp.zeros((HQ, HEAD_SIZE), jnp.float32)
    for c in range(n_kv):
        result = result + lanes_to_column(factors[c], on_diagonal) * merged_in[c, 0:HQ, :]
    result = result / lanes_to_column(amount, on_diagonal)
    out_ref[...] = result.astype(jnp.bfloat16)

    for early, leaf_sent, hub_sent in ((True, n_kv - 1, n_kv), (False, n_kv, n_kv - 1)):
        now = is_early if early else jnp.logical_not(is_early)

        @pl.when(jnp.logical_and(is_leaf, now))
        def _():
            arrived(q_col, leaf_sent, qs_sem.at[0])

        @pl.when(jnp.logical_and(is_hub, now))
        def _():
            arrived(q_col, hub_sent, qs_sem.at[0])

    @pl.when(is_leaf)
    def _():
        arrived(table, n_chip, ts_sem.at[0])
        arrived(part_send, n_chip, ps_sem.at[0])
        arrived(stat_send, n_chip, ss_sem.at[0])

    @pl.when(is_hub)
    def _():
        arrived(table, n_chip - 1, ts_sem.at[0])
        arrived(part_send, n_chip - 1, ps_sem.at[0])
        arrived(stat_send, n_chip - 1, ss_sem.at[0])
        arrived(q_send, n_req - 1, ds_sem.at[0])

    sends_near = jnp.logical_and(is_last, my_chip < n_near)

    @pl.when(jnp.logical_and(is_hub, jnp.logical_not(sends_near)))
    def _():
        arrived(merged, CORES * n_kv - 1, ms_sem.at[0])

    @pl.when(jnp.logical_and(is_hub, sends_near))
    def _():
        arrived(merged, CORES * n_kv - 1 - CORES, ms_sem.at[0])

    @pl.when(is_last)
    def _():
        arrived(near_send, n_near, ns_sem.at[0])
        arrived(part_send, n_near, ns_sem.at[1])


def solution(mesh):
    n_req, n_kv = mesh.shape["req"], mesh.shape["kv"]

    def on_device(queries, key_cache, value_cache, page_request, page_number, lengths):
        slots, page_tokens, width = key_cache.shape
        group = lengths.shape[0] // n_req
        n_chip = n_req // CORES
        dma = pltpu.SemaphoreType.DMA
        vmem = pl.BlockSpec(memory_space=pltpu.VMEM)
        anywhere = pl.BlockSpec(memory_space=pl.ANY)
        blob = (HQ + 2, HEAD_SIZE)
        attended = pl.pallas_call(
            functools.partial(kernel, n_req, n_kv, group),
            out_shape=pltpu.VMEM((HQ, HEAD_SIZE), jnp.bfloat16),
            in_specs=[anywhere] * 6,
            out_specs=vmem,
            scratch_shapes=[
                pltpu.SMEM(page_request.shape, jnp.int32),
                pltpu.SMEM(page_number.shape, jnp.int32),
                pltpu.SMEM(lengths.shape, jnp.int32),
                pltpu.VMEM(queries.shape, queries.dtype),
                pltpu.VMEM((slots, page_tokens, width), jnp.bfloat16),
                pltpu.VMEM((slots, page_tokens, width), jnp.bfloat16),
                pltpu.VMEM((HQ, HEAD_SIZE), jnp.float32),
                pltpu.VMEM((HQ, HEAD_SIZE), jnp.bfloat16),
                pltpu.VMEM((CORES * n_kv, HQ, HEAD_SIZE), jnp.bfloat16),
                pltpu.VMEM((n_req, 1, HEAD_SIZE), jnp.float32),
                pltpu.VMEM((CORES, n_req, 1, HEAD_SIZE), jnp.float32),
                pltpu.VMEM((n_req, CORES, HQ, HEAD_SIZE), jnp.bfloat16),
                pltpu.VMEM((n_chip, CORES, HQ, HEAD_SIZE), jnp.bfloat16),
                pltpu.VMEM((n_chip, CORES, HQ, HEAD_SIZE), jnp.int16),
                pltpu.VMEM((n_req, CORES, HQ, HEAD_SIZE), jnp.int16),
                pltpu.VMEM((n_chip, CORES, 3, HEAD_SIZE), jnp.float32),
                pltpu.VMEM((n_req, CORES, 3, HEAD_SIZE), jnp.float32),
                pltpu.VMEM((n_chip, CORES, 3, HEAD_SIZE), jnp.float32),
                pltpu.VMEM((n_req, HQ, HEAD_SIZE), jnp.int16),
                pltpu.VMEM((n_req, 3, HEAD_SIZE), jnp.float32),
                pltpu.VMEM((CORES * n_kv,) + blob, jnp.float32),
                pltpu.VMEM((n_kv,) + blob, jnp.float32),
                pltpu.SemaphoreType.REGULAR,
                pltpu.SemaphoreType.REGULAR,
                dma((4,)),
                dma((2,)),
                dma((1,)), dma((2,)),
                dma((1,)), dma((n_chip,)),
                dma((1,)), dma((n_chip,)),
                dma((1,)), dma((1,)),
                dma((1,)), dma((1,)),
                dma((2,)), dma((2,)),
                dma((1,)), dma((1,)),
            ],
            compiler_params=pltpu.CompilerParams(collective_id=0, has_side_effects=True),
        )(page_request, page_number, lengths, queries, key_cache, value_cache)
        return attended.reshape(queries.shape)

    placed = (
        P(("req", "kv"), None),
        P(("req", "kv"), None, None),
        P(("req", "kv"), None, None),
        P(("req", "kv")),
        P(("req", "kv")),
        P(),
    )
    return jax.shard_map(
        on_device, mesh=mesh, in_specs=placed, out_specs=P(("req", "kv"), None), check_vma=False
    )
```

```python
import functools

import jax
import jax.numpy as jnp
from jax import lax
from jax.experimental import pallas as pl
from jax.experimental.pallas import tpu as pltpu
from jax.sharding import PartitionSpec as P

HQ = 32
KEY_VALUE_HEADS = 8
HEAD_SIZE = 128
QUERY_PER_KV = 4
CORES = 2
PAIR = 2 * QUERY_PER_KV

lowest = -1e30
finest = 1e-30
STEPS = 32767.0
MESH = pl.DeviceIdType.MESH


def partners(me, n):
    if n & (n - 1):
        return [lax.rem(me + d, n) for d in range(n)]
    found = []
    for d in range(n):
        place, bit = me, 1
        while bit < n:
            if d & bit:
                place = place + bit - 2 * bit * lax.rem(lax.div(me, bit), 2)
            bit *= 2
        found.append(place)
    return found


def diagonal_to_lanes(column, on_diagonal):
    return jnp.sum(jnp.where(on_diagonal, column, 0.0), axis=0, keepdims=True)


def lanes_to_column(row, on_diagonal):
    return jnp.sum(jnp.where(on_diagonal, row, 0.0), axis=1, keepdims=True)


def kernel(
    n_req, n_kv, group,
    owner_hbm, number_hbm, length_hbm, q_hbm, key_hbm, value_hbm, out_ref,
    owner_ref, number_ref, length_ref, q_ref, keys, values, q_rows, q_own, q_col, table, held, q_send, q_in,
    part_send, part_in, stat_send, stat_in, near_send, near_in, near_stat, merged, merged_in,
    met_sem, far_sem, small_sem, page_sem, qs_sem, qr_sem, ts_sem, tr_sem, ds_sem, dr_sem, ps_sem, pr_sem, ss_sem, sr_sem, ns_sem, nr_sem, ms_sem, mr_sem,
):
    slots, page_tokens, _ = keys.shape
    n_chip = n_req // CORES
    n_second = max(3 * n_chip // 4, 1)
    my_req = lax.axis_index("req")
    my_kv = lax.axis_index("kv")
    my_chip = lax.div(my_req, CORES)
    core = lax.rem(my_req, CORES)
    is_hub = core == CORES - 1
    is_leaf = core < CORES - 1
    is_last = my_kv == n_kv - 1
    is_relay = my_kv == n_kv - 2
    is_early = my_kv < n_kv - 2
    is_near = my_kv == 0
    is_nearest = jnp.logical_and(my_kv == 0, my_chip < n_second)
    chip_peers = partners(my_chip, n_chip)
    kv_peers = partners(my_kv, n_kv)
    hub_of = [CORES * chip + CORES - 1 for chip in chip_peers]
    leaf_of = [CORES * chip for chip in chip_peers]

    small = [
        pltpu.make_async_copy(src, dst, small_sem.at[i])
        for i, (src, dst) in enumerate(
            ((owner_hbm, owner_ref), (q_hbm, q_ref), (number_hbm, number_ref), (length_hbm, length_ref))
        )
    ]
    for copy in small[:2]:
        copy.start()

    barrier = pltpu.get_barrier_semaphore()

    @pl.when(is_hub)
    def _():
        for z in range(n_kv - 1, -1, -1):

            @pl.when(jnp.logical_not(jnp.logical_and(is_last, z < n_kv - 2)))
            def _():
                pl.semaphore_signal(barrier, inc=1, device_id=(leaf_of[0], z), device_id_type=MESH)

        for d in range(n_chip - 1, 0, -1):
            pl.semaphore_signal(barrier, inc=1, device_id=(hub_of[d], my_kv), device_id_type=MESH)

    @pl.when(is_leaf)
    def _():
        pl.semaphore_signal(barrier, inc=1, device_id=(hub_of[0], my_kv), device_id_type=MESH)

    def remote(src, dst, send, recv, target):
        return pltpu.make_async_remote_copy(
            src_ref=src, dst_ref=dst, send_sem=send, recv_sem=recv,
            device_id=target, device_id_type=MESH,
        )

    def arrived(buffer, count, sem):
        if count:
            pltpu.make_async_copy(buffer.at[pl.ds(0, count)], buffer.at[pl.ds(0, count)], sem).wait()

    small[1].wait()
    for h in range(HQ):
        q_rows[h : h + 1, :] = q_ref[0:1, h * HEAD_SIZE : (h + 1) * HEAD_SIZE].astype(jnp.float32)
    q_own[...] = q_rows[...].astype(jnp.bfloat16)
    small[0].wait()
    lane1 = lax.broadcasted_iota(jnp.int32, (1, HEAD_SIZE), 1)
    own_table = jnp.full((1, HEAD_SIZE), -1.0, jnp.float32)
    for s in range(slots):
        own_table = jnp.where(lane1 == s, owner_ref[s].astype(jnp.float32), own_table)
    table[my_req] = own_table

    mine = core * n_kv + my_kv

    def send_query(last):
        for z in range(last, -1, -1):

            @pl.when(my_kv != z)
            def _():
                remote(q_own, q_col.at[mine], qs_sem.at[0], qr_sem.at[0], (hub_of[0], z)).start()

    def send_table():
        for d in range(n_chip - 1, 0, -1):
            remote(table.at[my_req], table.at[my_req], ts_sem.at[0], tr_sem.at[d], (hub_of[d], my_kv)).start()

    def leaf_column(early):
        pl.semaphore_wait(barrier, n_kv - 1 if early else n_kv)
        pl.semaphore_signal(met_sem, inc=1, device_id=(hub_of[0], my_kv), device_id_type=MESH)
        remote(q_own, q_col.at[mine], qs_sem.at[0], qr_sem.at[1], (hub_of[0], my_kv)).start()
        send_query(n_kv - 2 if early else n_kv - 1)

        @pl.when(is_relay)
        def _():
            for z in range(n_kv - 2):
                pl.semaphore_signal(far_sem, inc=1, device_id=(hub_of[0], z), device_id_type=MESH)

    def leaf_plane():
        pl.semaphore_wait(met_sem, 1)
        send_table()
        remote(table.at[my_req], table.at[my_req], ts_sem.at[0], tr_sem.at[0], (hub_of[0], my_kv)).start()

    def hub_column(early):
        pl.semaphore_wait(met_sem, 1)
        send_query(n_kv - 2 if early else n_kv - 1)
        if early:
            arrived(q_col, 1, qr_sem.at[1])
            pl.semaphore_wait(far_sem, 1)
            last = (hub_of[0], n_kv - 1)
            remote(q_own, q_col.at[mine], qs_sem.at[0], qr_sem.at[0], last).start()
            remote(q_col.at[my_kv], q_col.at[my_kv], qs_sem.at[0], qr_sem.at[0], last).start()

    def hub_plane():
        pl.semaphore_wait(barrier, n_chip)
        pl.semaphore_signal(met_sem, inc=1, device_id=(leaf_of[0], my_kv), device_id_type=MESH)
        send_table()

    for role, column, plane in ((is_leaf, leaf_column, leaf_plane), (is_hub, hub_column, hub_plane)):

        @pl.when(jnp.logical_and(role, jnp.logical_not(is_early)))
        def _():
            column(False)
            plane()

        @pl.when(jnp.logical_and(role, is_early))
        def _():
            plane()
            column(True)

    for copy in small[2:]:
        copy.start()
    for s in range(slots):
        pltpu.make_async_copy(key_hbm.at[s], keys.at[s], page_sem.at[0]).start()
        pltpu.make_async_copy(value_hbm.at[s], values.at[s], page_sem.at[1]).start()
    for copy in small[2:]:
        copy.wait()

    homes = []
    for d in range(n_chip):
        pair = []
        for b in range(CORES):
            index, present = jnp.int32(0), jnp.int32(0)
            for s in range(slots):
                same = lax.div(owner_ref[s], group) == d * CORES + b
                index = jnp.where(same, jnp.int32(s), index)
                present = jnp.where(same, jnp.int32(1), present)
            limit = length_ref[owner_ref[index]] - number_ref[index] * page_tokens
            place = jnp.where(present == 1, owner_ref[index] - (d * CORES + b) * group, -1)
            pair.append((index, limit * present, place))
        homes.append(pair)

    edges = [0, max(n_chip // 4, 1), max(3 * n_chip // 4, 1), n_chip]
    alone = [jnp.logical_and(is_hub, my_chip == c) for c in range(n_chip)]
    met = [jnp.logical_not(own) for own in alone]

    @pl.when(is_hub)
    def _():
        q_col[(CORES - 1) * n_kv + my_kv] = q_own[...]
        arrived(q_col, CORES * n_kv - 2, qr_sem.at[0])

        @pl.when(jnp.logical_not(is_early))
        def _():
            arrived(q_col, 1, qr_sem.at[1])

        choices = [q_col[c].astype(jnp.float32) for c in range(CORES * group)]
        for d in range(n_chip - 1, -1, -1):
            arrived(table, CORES if d else CORES - 1, tr_sem.at[d])
            picks = {}
            for a in range(CORES):
                row = table[leaf_of[d] + a]
                for b in range(CORES):
                    rel = row - ((leaf_of[0] + b) * group).astype(jnp.float32)
                    inside = jnp.logical_and(rel >= 0.0, rel < float(group))
                    picks[a, b] = jnp.max(jnp.where(inside, rel, -1.0), axis=1, keepdims=True)
            for a in range(CORES):
                for b in range(CORES):
                    held[b, leaf_of[d] + a] = jnp.broadcast_to(picks[a, b], (1, HEAD_SIZE))
                    pick = jnp.broadcast_to(picks[a, b], (HQ, HEAD_SIZE))
                    chosen = jnp.zeros((HQ, HEAD_SIZE), jnp.float32)
                    for c in range(group):
                        chosen = jnp.where(pick == float(c), choices[b * group + c], chosen)
                    if d == 0 and a == CORES - 1:
                        q_in[my_chip, b] = chosen.astype(jnp.bfloat16)
                    else:
                        q_send[d * CORES + a, b] = chosen.astype(jnp.bfloat16)
                if d or a < CORES - 1:
                    remote(
                        q_send.at[d * CORES + a], q_in.at[my_chip], ds_sem.at[0], dr_sem.at[my_chip],
                        (leaf_of[d] + a, my_kv),
                    ).start()

    pltpu.make_async_copy(key_hbm, keys, page_sem.at[0]).wait()
    pltpu.make_async_copy(value_hbm, values, page_sem.at[1]).wait()

    row = lax.broadcasted_iota(jnp.int32, (HQ, HEAD_SIZE), 0)
    lane = lax.broadcasted_iota(jnp.int32, (HQ, HEAD_SIZE), 1)
    on_diagonal = row == lane
    first = lax.broadcasted_iota(jnp.int32, (PAIR, HEAD_SIZE), 0) < QUERY_PER_KV
    token = lax.broadcasted_iota(jnp.int32, (HQ, page_tokens), 1)
    wide = 2 * HEAD_SIZE

    for stage, (low, high) in enumerate(zip(edges[:-1], edges[1:])):
        batch = [(c, b) for c in range(low, high) for b in range(CORES)]
        for c in range(low, high):

            @pl.when(met[c])
            def _():
                arrived(q_in, 1, dr_sem.at[c])

        scored = {}
        for d, b in batch:
            index, limit, _ = homes[d][b]
            query = q_in[d, b].astype(jnp.float32)
            pieces = []
            for k in range(HQ // PAIR):
                q8 = query[k * PAIR : (k + 1) * PAIR]
                both = jnp.concatenate(
                    [jnp.where(first, q8, 0.0), jnp.where(first, 0.0, q8)], axis=1
                ).astype(jnp.bfloat16)
                pieces.append(
                    lax.dot_general(
                        both, keys[index, :, k * wide : (k + 1) * wide],
                        (((1,), (1,)), ((), ())), preferred_element_type=jnp.float32,
                    )
                )
            scores = jnp.concatenate(pieces, axis=0) * HEAD_SIZE ** (-0.5)
            scored[d, b] = jnp.where(token < limit, scores, lowest)
        tops = {e: jnp.max(scored[e], axis=1, keepdims=True) for e in batch}
        weights = {e: jnp.exp(scored[e] - tops[e]) for e in batch}
        totals = {e: jnp.sum(weights[e], axis=1, keepdims=True) for e in batch}
        summed, largest = {}, {}
        for d, b in batch:
            index, _, _ = homes[d][b]
            blocks = []
            for k in range(HQ // PAIR):
                w8 = weights[d, b][k * PAIR : (k + 1) * PAIR].astype(jnp.bfloat16)
                both = jnp.dot(
                    w8, values[index, :, k * wide : (k + 1) * wide], preferred_element_type=jnp.float32
                )
                blocks.append(jnp.where(first, both[:, :HEAD_SIZE], both[:, HEAD_SIZE:]))
            blocks = jnp.concatenate(blocks, axis=0)
            largest[d, b] = jnp.maximum(jnp.max(jnp.abs(blocks), axis=1, keepdims=True), finest)
            summed[d, b] = blocks
        for d, b in batch:
            coded = jnp.round(summed[d, b] * (STEPS / largest[d, b]))
            part_send[d, b] = coded.astype(jnp.int32).astype(jnp.int16)
            lanes = [diagonal_to_lanes(column[d, b], on_diagonal) for column in (tops, totals, largest)]
            stat_send[d, b] = jnp.concatenate(lanes, axis=0)
            lanes[0] = jnp.where(homes[d][b][2] == 0, lanes[0], lowest)
            near_send[d, b] = jnp.concatenate(lanes, axis=0)
            if b < CORES - 1:
                continue
            target = (d * CORES + CORES - 1, my_kv)
            copy = remote(part_send.at[d], part_in.at[my_req], ps_sem.at[0], pr_sem.at[0], target)
            stat_copy = remote(stat_send.at[d], stat_in.at[my_req], ss_sem.at[0], sr_sem.at[0], target)

            for plane, chips in enumerate((n_chip, n_second)):
                if d >= chips:
                    continue

                @pl.when(my_kv == n_kv - 1 - plane)
                def _():
                    for a in range(CORES):
                        owner, e, k = (d * CORES + a, 0), plane * n_req + my_req, 2 * plane
                        remote(near_send.at[d, a], near_stat.at[e], ns_sem.at[k], nr_sem.at[k], owner).start()
                        remote(part_send.at[d, a], near_in.at[e], ns_sem.at[k + 1], nr_sem.at[k + 1], owner).start()

            @pl.when(met[d])
            def _():
                stat_copy.start()
                copy.start()


    sends_near = jnp.logical_or(is_last, jnp.logical_and(is_relay, my_chip < n_second))

    def send_merged(b, z):
        skipped = sends_near if z == 0 else jnp.bool_(False)
        if b == CORES - 1:
            skipped = jnp.logical_or(skipped, my_kv == z)

        @pl.when(jnp.logical_not(skipped))
        def _():
            remote(
                merged.at[b * n_kv + z], merged_in.at[my_kv], ms_sem.at[0], mr_sem.at[0], (leaf_of[0] + b, z)
            ).start()

    @pl.when(is_hub)
    def _():
        part_in[my_req] = part_send[my_chip]
        stat_in[my_req] = stat_send[my_chip]
        arrived(stat_in, n_req - 1, sr_sem.at[0])
        arrived(part_in, n_req - 1, pr_sem.at[0])
        for b in range(CORES):
            sources = [part_in.at[e, b] for e in range(n_req)]
            stats = [stat_in.at[e, b] for e in range(n_req)]
            tops = [stat[0:1, :] for stat in stats]
            totals = [stat[1:2, :] for stat in stats]
            steps = [stat[2:3, :] * (1.0 / STEPS) for stat in stats]
            picks = [held[b, e] for e in range(n_req)]
            member = [[picks[e] == float(c) for e in range(n_req)] for c in range(group)]
            merged_top, merged_total = [], []
            for c in range(group):
                best = jnp.full((1, HEAD_SIZE), lowest, jnp.float32)
                for e in range(n_req):
                    best = jnp.maximum(best, jnp.where(member[c][e], tops[e], lowest))
                merged_top.append(best)
            factors = []
            for e in range(n_req):
                best = tops[e]
                for c in range(group):
                    best = jnp.where(member[c][e], merged_top[c], best)
                factors.append(jnp.exp(tops[e] - best))
            for c in range(group):
                amount = jnp.zeros((1, HEAD_SIZE), jnp.float32)
                for e in range(n_req):
                    amount = amount + jnp.where(member[c][e], factors[e] * totals[e], 0.0)
                merged_total.append(amount)
            sums = [jnp.zeros((HQ, HEAD_SIZE), jnp.float32) for _ in range(group)]
            for e in range(n_req):
                coded = sources[e][...].astype(jnp.int32).astype(jnp.float32)
                scaled = lanes_to_column(factors[e] * steps[e], on_diagonal) * coded
                pick = jnp.broadcast_to(picks[e], (HQ, HEAD_SIZE))
                for c in range(group):
                    sums[c] = sums[c] + jnp.where(pick == float(c), scaled, 0.0)
            for c in range(group):
                merged[b * n_kv + c, 0:HQ, :] = sums[c]
                merged[b * n_kv + c, HQ : HQ + 2, :] = jnp.concatenate([merged_top[c], merged_total[c]], axis=0)
            send_merged(b, 0)

        for z in range(1, n_kv):
            for b in range(CORES):
                send_merged(b, z)
        merged_in[my_kv] = merged[(CORES - 1) * n_kv + my_kv]

    for role, others in ((is_leaf, n_kv), (is_hub, n_kv - 1)):

        @pl.when(jnp.logical_and(role, jnp.logical_not(is_near)))
        def _():
            arrived(merged_in, others, mr_sem.at[0])

        @pl.when(jnp.logical_and(role, jnp.logical_and(is_near, jnp.logical_not(is_nearest))))
        def _():
            arrived(merged_in, others - 1, mr_sem.at[0])

        @pl.when(jnp.logical_and(role, is_nearest))
        def _():
            arrived(merged_in, others - 2, mr_sem.at[0])

    def merge_near(plane):
        arrived(near_stat, n_req, nr_sem.at[2 * plane])
        some = range(plane * n_req, (plane + 1) * n_req)
        tops = {e: near_stat[e, 0:1, :] for e in some}
        best = functools.reduce(jnp.maximum, tops.values())
        factors = {e: jnp.exp(tops[e] - best) for e in some}
        amount = jnp.zeros((1, HEAD_SIZE), jnp.float32)
        for e in some:
            amount = amount + factors[e] * near_stat[e, 1:2, :]
        arrived(near_in, n_req, nr_sem.at[2 * plane + 1])
        total = jnp.zeros((HQ, HEAD_SIZE), jnp.float32)
        for e in some:
            step = factors[e] * (near_stat[e, 2:3, :] * (1.0 / STEPS))
            total = total + lanes_to_column(step, on_diagonal) * near_in[e].astype(jnp.int32).astype(jnp.float32)
        merged_in[n_kv - 1 - plane, 0:HQ, :] = total
        merged_in[n_kv - 1 - plane, HQ : HQ + 2, :] = jnp.concatenate([best, amount], axis=0)

    @pl.when(is_nearest)
    def _():
        merge_near(1)

    @pl.when(is_near)
    def _():
        merge_near(0)

    tops = [merged_in[c, HQ : HQ + 1, :] for c in range(n_kv)]
    best = tops[0]
    for c in range(1, n_kv):
        best = jnp.maximum(best, tops[c])
    factors = [jnp.exp(tops[c] - best) for c in range(n_kv)]
    amount = jnp.zeros((1, HEAD_SIZE), jnp.float32)
    for c in range(n_kv):
        amount = amount + factors[c] * merged_in[c, HQ + 1 : HQ + 2, :]
    result = jnp.zeros((HQ, HEAD_SIZE), jnp.float32)
    for c in range(n_kv):
        result = result + lanes_to_column(factors[c], on_diagonal) * merged_in[c, 0:HQ, :]
    result = result / lanes_to_column(amount, on_diagonal)
    out_ref[...] = result.astype(jnp.bfloat16)

    for early, leaf_sent, hub_sent in ((True, n_kv - 1, n_kv), (False, n_kv, n_kv - 1)):
        now = is_early if early else jnp.logical_not(is_early)

        @pl.when(jnp.logical_and(is_leaf, now))
        def _():
            arrived(q_col, leaf_sent, qs_sem.at[0])

        @pl.when(jnp.logical_and(is_hub, now))
        def _():
            arrived(q_col, hub_sent, qs_sem.at[0])

    @pl.when(is_leaf)
    def _():
        arrived(table, n_chip, ts_sem.at[0])
        arrived(part_send, n_chip, ps_sem.at[0])
        arrived(stat_send, n_chip, ss_sem.at[0])

    @pl.when(is_hub)
    def _():
        arrived(table, n_chip - 1, ts_sem.at[0])
        arrived(part_send, n_chip - 1, ps_sem.at[0])
        arrived(stat_send, n_chip - 1, ss_sem.at[0])
        arrived(q_send, n_req - 1, ds_sem.at[0])

    @pl.when(jnp.logical_and(is_hub, jnp.logical_not(sends_near)))
    def _():
        arrived(merged, CORES * n_kv - 1, ms_sem.at[0])

    @pl.when(jnp.logical_and(is_hub, sends_near))
    def _():
        arrived(merged, CORES * n_kv - 1 - CORES, ms_sem.at[0])

    for plane, chips in enumerate((n_chip, n_second)):

        @pl.when(my_kv == n_kv - 1 - plane)
        def _():
            arrived(near_send, chips, ns_sem.at[2 * plane])
            arrived(part_send, chips, ns_sem.at[2 * plane + 1])


def solution(mesh):
    n_req, n_kv = mesh.shape["req"], mesh.shape["kv"]

    def on_device(queries, key_cache, value_cache, page_request, page_number, lengths):
        slots, page_tokens, width = key_cache.shape
        group = lengths.shape[0] // n_req
        n_chip = n_req // CORES
        dma = pltpu.SemaphoreType.DMA
        vmem = pl.BlockSpec(memory_space=pltpu.VMEM)
        anywhere = pl.BlockSpec(memory_space=pl.ANY)
        blob = (HQ + 2, HEAD_SIZE)
        attended = pl.pallas_call(
            functools.partial(kernel, n_req, n_kv, group),
            out_shape=pltpu.VMEM((HQ, HEAD_SIZE), jnp.bfloat16),
            in_specs=[anywhere] * 6,
            out_specs=vmem,
            scratch_shapes=[
                pltpu.SMEM(page_request.shape, jnp.int32),
                pltpu.SMEM(page_number.shape, jnp.int32),
                pltpu.SMEM(lengths.shape, jnp.int32),
                pltpu.VMEM(queries.shape, queries.dtype),
                pltpu.VMEM((slots, page_tokens, width), jnp.bfloat16),
                pltpu.VMEM((slots, page_tokens, width), jnp.bfloat16),
                pltpu.VMEM((HQ, HEAD_SIZE), jnp.float32),
                pltpu.VMEM((HQ, HEAD_SIZE), jnp.bfloat16),
                pltpu.VMEM((CORES * n_kv, HQ, HEAD_SIZE), jnp.bfloat16),
                pltpu.VMEM((n_req, 1, HEAD_SIZE), jnp.float32),
                pltpu.VMEM((CORES, n_req, 1, HEAD_SIZE), jnp.float32),
                pltpu.VMEM((n_req, CORES, HQ, HEAD_SIZE), jnp.bfloat16),
                pltpu.VMEM((n_chip, CORES, HQ, HEAD_SIZE), jnp.bfloat16),
                pltpu.VMEM((n_chip, CORES, HQ, HEAD_SIZE), jnp.int16),
                pltpu.VMEM((n_req, CORES, HQ, HEAD_SIZE), jnp.int16),
                pltpu.VMEM((n_chip, CORES, 3, HEAD_SIZE), jnp.float32),
                pltpu.VMEM((n_req, CORES, 3, HEAD_SIZE), jnp.float32),
                pltpu.VMEM((n_chip, CORES, 3, HEAD_SIZE), jnp.float32),
                pltpu.VMEM((2 * n_req, HQ, HEAD_SIZE), jnp.int16),
                pltpu.VMEM((2 * n_req, 3, HEAD_SIZE), jnp.float32),
                pltpu.VMEM((CORES * n_kv,) + blob, jnp.float32),
                pltpu.VMEM((n_kv,) + blob, jnp.float32),
                pltpu.SemaphoreType.REGULAR,
                pltpu.SemaphoreType.REGULAR,
                dma((4,)),
                dma((2,)),
                dma((1,)), dma((2,)),
                dma((1,)), dma((n_chip,)),
                dma((1,)), dma((n_chip,)),
                dma((1,)), dma((1,)),
                dma((1,)), dma((1,)),
                dma((4,)), dma((4,)),
                dma((1,)), dma((1,)),
            ],
            compiler_params=pltpu.CompilerParams(collective_id=0, has_side_effects=True),
        )(page_request, page_number, lengths, queries, key_cache, value_cache)
        return attended.reshape(queries.shape)

    placed = (
        P(("req", "kv"), None),
        P(("req", "kv"), None, None),
        P(("req", "kv"), None, None),
        P(("req", "kv")),
        P(("req", "kv")),
        P(),
    )
    return jax.shard_map(
        on_device, mesh=mesh, in_specs=placed, out_specs=P(("req", "kv"), None), check_vma=False
    )
```

```python
import functools

import jax
import jax.numpy as jnp
from jax import lax
from jax.experimental import pallas as pl
from jax.experimental.pallas import tpu as pltpu
from jax.sharding import PartitionSpec as P

HQ = 32
KEY_VALUE_HEADS = 8
HEAD_SIZE = 128
QUERY_PER_KV = 4
CORES = 2
PAIR = 2 * QUERY_PER_KV

lowest = -1e30
finest = 2.0 ** -126
STEPS = 32767.0
MESH = pl.DeviceIdType.MESH


def partners(me, n):
    if n & (n - 1):
        return [lax.rem(me + d, n) for d in range(n)]
    found = []
    for d in range(n):
        place, bit = me, 1
        while bit < n:
            if d & bit:
                place = place + bit - 2 * bit * lax.rem(lax.div(me, bit), 2)
            bit *= 2
        found.append(place)
    return found


def diagonal_to_lanes(column, on_diagonal):
    return jnp.sum(jnp.where(on_diagonal, column, 0.0), axis=0, keepdims=True)


def lanes_to_column(row, on_diagonal):
    return jnp.sum(jnp.where(on_diagonal, row, 0.0), axis=1, keepdims=True)


def kernel(
    n_req, n_kv, group,
    owner_hbm, number_hbm, length_hbm, q_hbm, key_hbm, value_hbm, out_ref,
    owner_ref, number_ref, length_ref, q_ref, keys, values, q_rows, q_own, q_col, table, held, q_send, q_in,
    part_send, part_in, stat_send, stat_in, near_send, near_in, near_stat, merged, merged_in,
    met_sem, far_sem, small_sem, page_sem, qs_sem, qr_sem, ts_sem, tr_sem, ds_sem, dr_sem, ps_sem, pr_sem, ss_sem, sr_sem, ns_sem, nr_sem, ms_sem, mr_sem,
):
    slots, page_tokens, _ = keys.shape
    n_chip = n_req // CORES
    n_second = max(3 * n_chip // 4, 1)
    my_req = lax.axis_index("req")
    my_kv = lax.axis_index("kv")
    my_chip = lax.div(my_req, CORES)
    core = lax.rem(my_req, CORES)
    is_hub = core == CORES - 1
    is_leaf = core < CORES - 1
    is_last = my_kv == n_kv - 1
    is_relay = my_kv == n_kv - 2
    is_early = my_kv < n_kv - 2
    is_near = my_kv == 0
    is_nearest = jnp.logical_and(my_kv == 0, my_chip < n_second)
    chip_peers = partners(my_chip, n_chip)
    kv_peers = partners(my_kv, n_kv)
    hub_of = [CORES * chip + CORES - 1 for chip in chip_peers]
    leaf_of = [CORES * chip for chip in chip_peers]

    small = [
        pltpu.make_async_copy(src, dst, small_sem.at[i])
        for i, (src, dst) in enumerate(
            ((owner_hbm, owner_ref), (q_hbm, q_ref), (number_hbm, number_ref), (length_hbm, length_ref))
        )
    ]
    for copy in small[:2]:
        copy.start()

    barrier = pltpu.get_barrier_semaphore()

    @pl.when(is_hub)
    def _():
        for z in range(n_kv - 1, -1, -1):

            @pl.when(jnp.logical_not(jnp.logical_and(is_last, z < n_kv - 2)))
            def _():
                pl.semaphore_signal(barrier, inc=1, device_id=(leaf_of[0], z), device_id_type=MESH)

        for d in range(n_chip - 1, 0, -1):
            pl.semaphore_signal(barrier, inc=1, device_id=(hub_of[d], my_kv), device_id_type=MESH)

    @pl.when(is_leaf)
    def _():
        pl.semaphore_signal(barrier, inc=1, device_id=(hub_of[0], my_kv), device_id_type=MESH)

    def remote(src, dst, send, recv, target):
        return pltpu.make_async_remote_copy(
            src_ref=src, dst_ref=dst, send_sem=send, recv_sem=recv,
            device_id=target, device_id_type=MESH,
        )

    def arrived(buffer, count, sem):
        if count:
            pltpu.make_async_copy(buffer.at[pl.ds(0, count)], buffer.at[pl.ds(0, count)], sem).wait()

    small[1].wait()
    for h in range(HQ):
        q_rows[h : h + 1, :] = q_ref[0:1, h * HEAD_SIZE : (h + 1) * HEAD_SIZE].astype(jnp.float32)
    q_own[...] = q_rows[...].astype(jnp.bfloat16)
    small[0].wait()
    lane1 = lax.broadcasted_iota(jnp.int32, (1, HEAD_SIZE), 1)
    own_table = jnp.full((1, HEAD_SIZE), -1.0, jnp.float32)
    for s in range(slots):
        own_table = jnp.where(lane1 == s, owner_ref[s].astype(jnp.float32), own_table)
    table[my_req] = own_table

    mine = core * n_kv + my_kv

    def send_query(last):
        for z in range(last, -1, -1):

            @pl.when(my_kv != z)
            def _():
                remote(q_own, q_col.at[mine], qs_sem.at[0], qr_sem.at[0], (hub_of[0], z)).start()

    def send_table():
        for d in range(n_chip - 1, 0, -1):
            remote(table.at[my_req], table.at[my_req], ts_sem.at[0], tr_sem.at[d], (hub_of[d], my_kv)).start()

    def leaf_column(early):
        pl.semaphore_wait(barrier, n_kv - 1 if early else n_kv)
        pl.semaphore_signal(met_sem, inc=1, device_id=(hub_of[0], my_kv), device_id_type=MESH)

        @pl.when(is_relay)
        def _():
            for z in range(n_kv - 2):
                pl.semaphore_signal(far_sem, inc=1, device_id=(hub_of[0], z), device_id_type=MESH)

        remote(q_own, q_col.at[mine], qs_sem.at[0], qr_sem.at[1], (hub_of[0], my_kv)).start()
        send_query(n_kv - 2 if early else n_kv - 1)

    def leaf_plane():
        pl.semaphore_wait(met_sem, 1)
        send_table()
        remote(table.at[my_req], table.at[my_req], ts_sem.at[0], tr_sem.at[0], (hub_of[0], my_kv)).start()

    def hub_column(early):
        pl.semaphore_wait(met_sem, 1)
        send_query(n_kv - 2 if early else n_kv - 1)
        if early:
            arrived(q_col, 1, qr_sem.at[1])
            pl.semaphore_wait(far_sem, 1)
            last = (hub_of[0], n_kv - 1)
            remote(q_own, q_col.at[mine], qs_sem.at[0], qr_sem.at[0], last).start()
            remote(q_col.at[my_kv], q_col.at[my_kv], qs_sem.at[0], qr_sem.at[0], last).start()

    def hub_plane():
        pl.semaphore_wait(barrier, n_chip)
        pl.semaphore_signal(met_sem, inc=1, device_id=(leaf_of[0], my_kv), device_id_type=MESH)
        send_table()

    for role, column, plane in ((is_leaf, leaf_column, leaf_plane), (is_hub, hub_column, hub_plane)):

        @pl.when(jnp.logical_and(role, jnp.logical_not(is_early)))
        def _():
            column(False)
            plane()

        @pl.when(jnp.logical_and(role, is_early))
        def _():
            plane()
            column(True)

    for copy in small[2:]:
        copy.start()
    for s in range(slots):
        pltpu.make_async_copy(key_hbm.at[s], keys.at[s], page_sem.at[0]).start()
        pltpu.make_async_copy(value_hbm.at[s], values.at[s], page_sem.at[1]).start()
    for copy in small[2:]:
        copy.wait()

    homes = []
    for d in range(n_chip):
        pair = []
        for b in range(CORES):
            index, present = jnp.int32(0), jnp.int32(0)
            for s in range(slots):
                same = lax.div(owner_ref[s], group) == d * CORES + b
                index = jnp.where(same, jnp.int32(s), index)
                present = jnp.where(same, jnp.int32(1), present)
            limit = length_ref[owner_ref[index]] - number_ref[index] * page_tokens
            place = jnp.where(present == 1, owner_ref[index] - (d * CORES + b) * group, -1)
            pair.append((index, limit * present, place))
        homes.append(pair)

    edges = [0, max(n_chip // 4, 1), max(3 * n_chip // 4, 1), n_chip]
    alone = [jnp.logical_and(is_hub, my_chip == c) for c in range(n_chip)]
    met = [jnp.logical_not(own) for own in alone]

    @pl.when(is_hub)
    def _():
        q_col[(CORES - 1) * n_kv + my_kv] = q_own[...]
        arrived(q_col, CORES * n_kv - 2, qr_sem.at[0])

        @pl.when(jnp.logical_not(is_early))
        def _():
            arrived(q_col, 1, qr_sem.at[1])

        choices = [q_col[c].astype(jnp.float32) for c in range(CORES * group)]
        for d in range(n_chip - 1, -1, -1):
            arrived(table, CORES if d else CORES - 1, tr_sem.at[d])
            picks = {}
            for a in range(CORES):
                row = table[leaf_of[d] + a]
                for b in range(CORES):
                    rel = row - ((leaf_of[0] + b) * group).astype(jnp.float32)
                    inside = jnp.logical_and(rel >= 0.0, rel < float(group))
                    picks[a, b] = jnp.max(jnp.where(inside, rel, -1.0), axis=1, keepdims=True)
            for a in range(CORES):
                for b in range(CORES):
                    held[b, leaf_of[d] + a] = jnp.broadcast_to(picks[a, b], (1, HEAD_SIZE))
                    pick = jnp.broadcast_to(picks[a, b], (HQ, HEAD_SIZE))
                    chosen = jnp.zeros((HQ, HEAD_SIZE), jnp.float32)
                    for c in range(group):
                        chosen = jnp.where(pick == float(c), choices[b * group + c], chosen)
                    if d == 0 and a == CORES - 1:
                        q_in[my_chip, b] = chosen.astype(jnp.bfloat16)
                    else:
                        q_send[d * CORES + a, b] = chosen.astype(jnp.bfloat16)
                if d or a < CORES - 1:
                    remote(
                        q_send.at[d * CORES + a], q_in.at[my_chip], ds_sem.at[0], dr_sem.at[my_chip],
                        (leaf_of[d] + a, my_kv),
                    ).start()

    pltpu.make_async_copy(key_hbm, keys, page_sem.at[0]).wait()
    pltpu.make_async_copy(value_hbm, values, page_sem.at[1]).wait()

    row = lax.broadcasted_iota(jnp.int32, (HQ, HEAD_SIZE), 0)
    lane = lax.broadcasted_iota(jnp.int32, (HQ, HEAD_SIZE), 1)
    on_diagonal = row == lane
    first = lax.broadcasted_iota(jnp.int32, (PAIR, HEAD_SIZE), 0) < QUERY_PER_KV
    token = lax.broadcasted_iota(jnp.int32, (HQ, page_tokens), 1)
    wide = 2 * HEAD_SIZE

    for stage, (low, high) in enumerate(zip(edges[:-1], edges[1:])):
        batch = [(c, b) for c in range(low, high) for b in range(CORES)]
        for c in range(low, high):

            @pl.when(met[c])
            def _():
                arrived(q_in, 1, dr_sem.at[c])

        scored = {}
        for d, b in batch:
            index, limit, _ = homes[d][b]
            query = q_in[d, b].astype(jnp.float32)
            pieces = []
            for k in range(HQ // PAIR):
                q8 = query[k * PAIR : (k + 1) * PAIR]
                both = jnp.concatenate(
                    [jnp.where(first, q8, 0.0), jnp.where(first, 0.0, q8)], axis=1
                ).astype(jnp.bfloat16)
                pieces.append(
                    lax.dot_general(
                        both, keys[index, :, k * wide : (k + 1) * wide],
                        (((1,), (1,)), ((), ())), preferred_element_type=jnp.float32,
                    )
                )
            scores = jnp.concatenate(pieces, axis=0) * HEAD_SIZE ** (-0.5)
            scored[d, b] = jnp.where(token < limit, scores, lowest)
        tops = {e: jnp.max(scored[e], axis=1, keepdims=True) for e in batch}
        weights = {e: jnp.exp(scored[e] - tops[e]) for e in batch}
        totals = {e: jnp.sum(weights[e], axis=1, keepdims=True) for e in batch}
        summed, largest = {}, {}
        for d, b in batch:
            index, _, _ = homes[d][b]
            blocks = []
            for k in range(HQ // PAIR):
                w8 = weights[d, b][k * PAIR : (k + 1) * PAIR].astype(jnp.bfloat16)
                both = jnp.dot(
                    w8, values[index, :, k * wide : (k + 1) * wide], preferred_element_type=jnp.float32
                )
                blocks.append(jnp.where(first, both[:, :HEAD_SIZE], both[:, HEAD_SIZE:]))
            blocks = jnp.concatenate(blocks, axis=0)
            largest[d, b] = jnp.maximum(jnp.max(jnp.abs(blocks), axis=1, keepdims=True), finest)
            summed[d, b] = blocks
        for d, b in batch:
            coded = jnp.round(summed[d, b] * (1.0 / largest[d, b]) * STEPS)
            part_send[d, b] = coded.astype(jnp.int32).astype(jnp.int16)
            lanes = [diagonal_to_lanes(column[d, b], on_diagonal) for column in (tops, totals, largest)]
            stat_send[d, b] = jnp.concatenate(lanes, axis=0)
            lanes[0] = jnp.where(homes[d][b][2] == 0, lanes[0], lowest)
            near_send[d, b] = jnp.concatenate(lanes, axis=0)
            if b < CORES - 1:
                continue
            target = (d * CORES + CORES - 1, my_kv)
            copy = remote(part_send.at[d], part_in.at[my_req], ps_sem.at[0], pr_sem.at[0], target)
            stat_copy = remote(stat_send.at[d], stat_in.at[my_req], ss_sem.at[0], sr_sem.at[0], target)

            for plane, chips in enumerate((n_chip, n_second)):
                if d >= chips:
                    continue

                @pl.when(my_kv == n_kv - 1 - plane)
                def _():
                    for a in range(CORES):
                        owner, e, k = (d * CORES + a, 0), plane * n_req + my_req, 2 * plane
                        remote(near_send.at[d, a], near_stat.at[e], ns_sem.at[k], nr_sem.at[k], owner).start()
                        remote(part_send.at[d, a], near_in.at[e], ns_sem.at[k + 1], nr_sem.at[k + 1], owner).start()

            @pl.when(met[d])
            def _():
                stat_copy.start()
                copy.start()


    sends_near = jnp.logical_or(is_last, jnp.logical_and(is_relay, my_chip < n_second))

    def send_merged(b, z):
        skipped = sends_near if z == 0 else jnp.bool_(False)
        if b == CORES - 1:
            skipped = jnp.logical_or(skipped, my_kv == z)

        @pl.when(jnp.logical_not(skipped))
        def _():
            remote(
                merged.at[b * n_kv + z], merged_in.at[my_kv], ms_sem.at[0], mr_sem.at[0], (leaf_of[0] + b, z)
            ).start()

    @pl.when(is_hub)
    def _():
        part_in[my_req] = part_send[my_chip]
        stat_in[my_req] = stat_send[my_chip]
        arrived(stat_in, n_req - 1, sr_sem.at[0])
        arrived(part_in, n_req - 1, pr_sem.at[0])
        for b in range(CORES):
            sources = [part_in.at[e, b] for e in range(n_req)]
            stats = [stat_in.at[e, b] for e in range(n_req)]
            tops = [stat[0:1, :] for stat in stats]
            totals = [stat[1:2, :] for stat in stats]
            scales = [stat[2:3, :] for stat in stats]
            picks = [held[b, e] for e in range(n_req)]
            member = [[picks[e] == float(c) for e in range(n_req)] for c in range(group)]
            merged_top, merged_total = [], []
            for c in range(group):
                best = jnp.full((1, HEAD_SIZE), lowest, jnp.float32)
                for e in range(n_req):
                    best = jnp.maximum(best, jnp.where(member[c][e], tops[e], lowest))
                merged_top.append(best)
            factors = []
            for e in range(n_req):
                best = tops[e]
                for c in range(group):
                    best = jnp.where(member[c][e], merged_top[c], best)
                factors.append(jnp.exp(tops[e] - best))
            for c in range(group):
                amount = jnp.zeros((1, HEAD_SIZE), jnp.float32)
                for e in range(n_req):
                    amount = amount + jnp.where(member[c][e], factors[e] * totals[e], 0.0)
                merged_total.append(amount)
            sums = [jnp.zeros((HQ, HEAD_SIZE), jnp.float32) for _ in range(group)]
            for e in range(n_req):
                coded = sources[e][...].astype(jnp.int32).astype(jnp.float32) * (1.0 / STEPS)
                scaled = lanes_to_column(factors[e] * scales[e], on_diagonal) * coded
                pick = jnp.broadcast_to(picks[e], (HQ, HEAD_SIZE))
                for c in range(group):
                    sums[c] = sums[c] + jnp.where(pick == float(c), scaled, 0.0)
            for c in range(group):
                merged[b * n_kv + c, 0:HQ, :] = sums[c]
                merged[b * n_kv + c, HQ : HQ + 2, :] = jnp.concatenate([merged_top[c], merged_total[c]], axis=0)
            send_merged(b, 0)

        for z in range(1, n_kv):
            for b in range(CORES):
                send_merged(b, z)
        merged_in[my_kv] = merged[(CORES - 1) * n_kv + my_kv]

    for role, others in ((is_leaf, n_kv), (is_hub, n_kv - 1)):

        @pl.when(jnp.logical_and(role, jnp.logical_not(is_near)))
        def _():
            arrived(merged_in, others, mr_sem.at[0])

        @pl.when(jnp.logical_and(role, jnp.logical_and(is_near, jnp.logical_not(is_nearest))))
        def _():
            arrived(merged_in, others - 1, mr_sem.at[0])

        @pl.when(jnp.logical_and(role, is_nearest))
        def _():
            arrived(merged_in, others - 2, mr_sem.at[0])

    def merge_near(plane):
        arrived(near_stat, n_req, nr_sem.at[2 * plane])
        some = range(plane * n_req, (plane + 1) * n_req)
        tops = {e: near_stat[e, 0:1, :] for e in some}
        best = functools.reduce(jnp.maximum, tops.values())
        factors = {e: jnp.exp(tops[e] - best) for e in some}
        amount = jnp.zeros((1, HEAD_SIZE), jnp.float32)
        for e in some:
            amount = amount + factors[e] * near_stat[e, 1:2, :]
        arrived(near_in, n_req, nr_sem.at[2 * plane + 1])
        total = jnp.zeros((HQ, HEAD_SIZE), jnp.float32)
        for e in some:
            coded = near_in[e].astype(jnp.int32).astype(jnp.float32) * (1.0 / STEPS)
            total = total + lanes_to_column(factors[e] * near_stat[e, 2:3, :], on_diagonal) * coded
        merged_in[n_kv - 1 - plane, 0:HQ, :] = total
        merged_in[n_kv - 1 - plane, HQ : HQ + 2, :] = jnp.concatenate([best, amount], axis=0)

    @pl.when(is_nearest)
    def _():
        merge_near(1)

    @pl.when(is_near)
    def _():
        merge_near(0)

    tops = [merged_in[c, HQ : HQ + 1, :] for c in range(n_kv)]
    best = tops[0]
    for c in range(1, n_kv):
        best = jnp.maximum(best, tops[c])
    factors = [jnp.exp(tops[c] - best) for c in range(n_kv)]
    amount = jnp.zeros((1, HEAD_SIZE), jnp.float32)
    for c in range(n_kv):
        amount = amount + factors[c] * merged_in[c, HQ + 1 : HQ + 2, :]
    result = jnp.zeros((HQ, HEAD_SIZE), jnp.float32)
    for c in range(n_kv):
        result = result + lanes_to_column(factors[c], on_diagonal) * merged_in[c, 0:HQ, :]
    result = result / lanes_to_column(amount, on_diagonal)
    out_ref[...] = result.astype(jnp.bfloat16)

    for early, leaf_sent, hub_sent in ((True, n_kv - 1, n_kv), (False, n_kv, n_kv - 1)):
        now = is_early if early else jnp.logical_not(is_early)

        @pl.when(jnp.logical_and(is_leaf, now))
        def _():
            arrived(q_col, leaf_sent, qs_sem.at[0])

        @pl.when(jnp.logical_and(is_hub, now))
        def _():
            arrived(q_col, hub_sent, qs_sem.at[0])

    @pl.when(is_leaf)
    def _():
        arrived(table, n_chip, ts_sem.at[0])
        arrived(part_send, n_chip, ps_sem.at[0])
        arrived(stat_send, n_chip, ss_sem.at[0])

    @pl.when(is_hub)
    def _():
        arrived(table, n_chip - 1, ts_sem.at[0])
        arrived(part_send, n_chip - 1, ps_sem.at[0])
        arrived(stat_send, n_chip - 1, ss_sem.at[0])
        arrived(q_send, n_req - 1, ds_sem.at[0])

    @pl.when(jnp.logical_and(is_hub, jnp.logical_not(sends_near)))
    def _():
        arrived(merged, CORES * n_kv - 1, ms_sem.at[0])

    @pl.when(jnp.logical_and(is_hub, sends_near))
    def _():
        arrived(merged, CORES * n_kv - 1 - CORES, ms_sem.at[0])

    for plane, chips in enumerate((n_chip, n_second)):

        @pl.when(my_kv == n_kv - 1 - plane)
        def _():
            arrived(near_send, chips, ns_sem.at[2 * plane])
            arrived(part_send, chips, ns_sem.at[2 * plane + 1])


def solution(mesh):
    n_req, n_kv = mesh.shape["req"], mesh.shape["kv"]

    def on_device(queries, key_cache, value_cache, page_request, page_number, lengths):
        slots, page_tokens, width = key_cache.shape
        group = lengths.shape[0] // n_req
        n_chip = n_req // CORES
        dma = pltpu.SemaphoreType.DMA
        vmem = pl.BlockSpec(memory_space=pltpu.VMEM)
        anywhere = pl.BlockSpec(memory_space=pl.ANY)
        blob = (HQ + 2, HEAD_SIZE)
        attended = pl.pallas_call(
            functools.partial(kernel, n_req, n_kv, group),
            out_shape=pltpu.VMEM((HQ, HEAD_SIZE), jnp.bfloat16),
            in_specs=[anywhere] * 6,
            out_specs=vmem,
            scratch_shapes=[
                pltpu.SMEM(page_request.shape, jnp.int32),
                pltpu.SMEM(page_number.shape, jnp.int32),
                pltpu.SMEM(lengths.shape, jnp.int32),
                pltpu.VMEM(queries.shape, queries.dtype),
                pltpu.VMEM((slots, page_tokens, width), jnp.bfloat16),
                pltpu.VMEM((slots, page_tokens, width), jnp.bfloat16),
                pltpu.VMEM((HQ, HEAD_SIZE), jnp.float32),
                pltpu.VMEM((HQ, HEAD_SIZE), jnp.bfloat16),
                pltpu.VMEM((CORES * n_kv, HQ, HEAD_SIZE), jnp.bfloat16),
                pltpu.VMEM((n_req, 1, HEAD_SIZE), jnp.float32),
                pltpu.VMEM((CORES, n_req, 1, HEAD_SIZE), jnp.float32),
                pltpu.VMEM((n_req, CORES, HQ, HEAD_SIZE), jnp.bfloat16),
                pltpu.VMEM((n_chip, CORES, HQ, HEAD_SIZE), jnp.bfloat16),
                pltpu.VMEM((n_chip, CORES, HQ, HEAD_SIZE), jnp.int16),
                pltpu.VMEM((n_req, CORES, HQ, HEAD_SIZE), jnp.int16),
                pltpu.VMEM((n_chip, CORES, 3, HEAD_SIZE), jnp.float32),
                pltpu.VMEM((n_req, CORES, 3, HEAD_SIZE), jnp.float32),
                pltpu.VMEM((n_chip, CORES, 3, HEAD_SIZE), jnp.float32),
                pltpu.VMEM((2 * n_req, HQ, HEAD_SIZE), jnp.int16),
                pltpu.VMEM((2 * n_req, 3, HEAD_SIZE), jnp.float32),
                pltpu.VMEM((CORES * n_kv,) + blob, jnp.float32),
                pltpu.VMEM((n_kv,) + blob, jnp.float32),
                pltpu.SemaphoreType.REGULAR,
                pltpu.SemaphoreType.REGULAR,
                dma((4,)),
                dma((2,)),
                dma((1,)), dma((2,)),
                dma((1,)), dma((n_chip,)),
                dma((1,)), dma((n_chip,)),
                dma((1,)), dma((1,)),
                dma((1,)), dma((1,)),
                dma((4,)), dma((4,)),
                dma((1,)), dma((1,)),
            ],
            compiler_params=pltpu.CompilerParams(collective_id=0, has_side_effects=True),
        )(page_request, page_number, lengths, queries, key_cache, value_cache)
        return attended.reshape(queries.shape)

    placed = (
        P(("req", "kv"), None),
        P(("req", "kv"), None, None),
        P(("req", "kv"), None, None),
        P(("req", "kv")),
        P(("req", "kv")),
        P(),
    )
    return jax.shard_map(
        on_device, mesh=mesh, in_specs=placed, out_specs=P(("req", "kv"), None), check_vma=False
    )
```

```python
import functools

import jax
import jax.numpy as jnp
from jax import lax
from jax.experimental import pallas as pl
from jax.experimental.pallas import tpu as pltpu
from jax.sharding import PartitionSpec as P

HQ = 32
KEY_VALUE_HEADS = 8
HEAD_SIZE = 128
QUERY_PER_KV = 4
CORES = 2
PAIR = 2 * QUERY_PER_KV

lowest = -1e30
finest = 2.0 ** -126
STEPS = 32767.0
MESH = pl.DeviceIdType.MESH


def partners(me, n):
    if n & (n - 1):
        return [lax.rem(me + d, n) for d in range(n)]
    found = []
    for d in range(n):
        place, bit = me, 1
        while bit < n:
            if d & bit:
                place = place + bit - 2 * bit * lax.rem(lax.div(me, bit), 2)
            bit *= 2
        found.append(place)
    return found


def diagonal_to_lanes(column, on_diagonal):
    return jnp.sum(jnp.where(on_diagonal, column, 0.0), axis=0, keepdims=True)


def lanes_to_column(row, on_diagonal):
    return jnp.sum(jnp.where(on_diagonal, row, 0.0), axis=1, keepdims=True)


def kernel(
    n_req, n_kv, group,
    owner_hbm, number_hbm, length_hbm, q_hbm, key_hbm, value_hbm, out_ref,
    owner_ref, number_ref, length_ref, q_ref, keys, values, q_rows, q_own, q_col, table, held, q_send, q_in,
    part_send, part_in, stat_send, stat_in, near_send, near_in, near_stat, merged, merged_in,
    met_sem, far_sem, small_sem, page_sem, qs_sem, qr_sem, ts_sem, tr_sem, ds_sem, dr_sem, ps_sem, pr_sem, ss_sem, sr_sem, ns_sem, nr_sem, ms_sem, mr_sem,
):
    slots, page_tokens, _ = keys.shape
    n_chip = n_req // CORES
    n_second = max(3 * n_chip // 4, 1)
    my_req = lax.axis_index("req")
    my_kv = lax.axis_index("kv")
    my_chip = lax.div(my_req, CORES)
    core = lax.rem(my_req, CORES)
    is_hub = core == CORES - 1
    is_leaf = core < CORES - 1
    is_last = my_kv == n_kv - 1
    is_relay = my_kv == n_kv - 2
    is_early = my_kv < n_kv - 2
    is_near = my_kv == 0
    is_nearest = jnp.logical_and(my_kv == 0, my_chip < n_second)
    chip_peers = partners(my_chip, n_chip)
    kv_peers = partners(my_kv, n_kv)
    hub_of = [CORES * chip + CORES - 1 for chip in chip_peers]
    leaf_of = [CORES * chip for chip in chip_peers]

    small = [
        pltpu.make_async_copy(src, dst, small_sem.at[i])
        for i, (src, dst) in enumerate(
            ((owner_hbm, owner_ref), (q_hbm, q_ref), (number_hbm, number_ref), (length_hbm, length_ref))
        )
    ]
    for copy in small[:2]:
        copy.start()

    barrier = pltpu.get_barrier_semaphore()

    @pl.when(is_hub)
    def _():
        for z in range(n_kv - 1, -1, -1):

            @pl.when(jnp.logical_not(jnp.logical_and(is_last, z < n_kv - 2)))
            def _():
                pl.semaphore_signal(barrier, inc=1, device_id=(leaf_of[0], z), device_id_type=MESH)

        for d in range(n_chip - 1, 0, -1):
            pl.semaphore_signal(barrier, inc=1, device_id=(hub_of[d], my_kv), device_id_type=MESH)

    @pl.when(is_leaf)
    def _():
        pl.semaphore_signal(barrier, inc=1, device_id=(hub_of[0], my_kv), device_id_type=MESH)

    def remote(src, dst, send, recv, target):
        return pltpu.make_async_remote_copy(
            src_ref=src, dst_ref=dst, send_sem=send, recv_sem=recv,
            device_id=target, device_id_type=MESH,
        )

    def arrived(buffer, count, sem):
        if count:
            pltpu.make_async_copy(buffer.at[pl.ds(0, count)], buffer.at[pl.ds(0, count)], sem).wait()

    small[1].wait()
    for h in range(HQ):
        q_rows[h : h + 1, :] = q_ref[0:1, h * HEAD_SIZE : (h + 1) * HEAD_SIZE].astype(jnp.float32)
    q_own[...] = q_rows[...].astype(jnp.bfloat16)
    small[0].wait()
    lane1 = lax.broadcasted_iota(jnp.int32, (1, HEAD_SIZE), 1)
    own_table = jnp.full((1, HEAD_SIZE), -1.0, jnp.float32)
    for s in range(slots):
        own_table = jnp.where(lane1 == s, owner_ref[s].astype(jnp.float32), own_table)
    table[my_req] = own_table

    mine = core * n_kv + my_kv

    def send_query(last):
        for z in range(last, -1, -1):

            @pl.when(my_kv != z)
            def _():
                remote(q_own, q_col.at[mine], qs_sem.at[0], qr_sem.at[0], (hub_of[0], z)).start()

    def send_table():
        for d in range(n_chip - 1, 0, -1):
            remote(table.at[my_req], table.at[my_req], ts_sem.at[0], tr_sem.at[d], (hub_of[d], my_kv)).start()

    def leaf_column(early):
        pl.semaphore_wait(barrier, n_kv - 1 if early else n_kv)
        pl.semaphore_signal(met_sem, inc=1, device_id=(hub_of[0], my_kv), device_id_type=MESH)

        @pl.when(is_relay)
        def _():
            for z in range(n_kv - 2):
                pl.semaphore_signal(far_sem, inc=1, device_id=(hub_of[0], z), device_id_type=MESH)

        remote(q_own, q_col.at[mine], qs_sem.at[0], qr_sem.at[1], (hub_of[0], my_kv)).start()
        send_query(n_kv - 2 if early else n_kv - 1)

    def leaf_plane():
        pl.semaphore_wait(met_sem, 1)
        send_table()
        remote(table.at[my_req], table.at[my_req], ts_sem.at[0], tr_sem.at[0], (hub_of[0], my_kv)).start()

    def hub_column(early):
        pl.semaphore_wait(met_sem, 1)
        send_query(n_kv - 2 if early else n_kv - 1)
        if early:
            arrived(q_col, 1, qr_sem.at[1])
            pl.semaphore_wait(far_sem, 1)
            last = (hub_of[0], n_kv - 1)
            remote(q_own, q_col.at[mine], qs_sem.at[0], qr_sem.at[0], last).start()
            remote(q_col.at[my_kv], q_col.at[my_kv], qs_sem.at[0], qr_sem.at[0], last).start()

    def hub_plane():
        pl.semaphore_wait(barrier, n_chip)
        pl.semaphore_signal(met_sem, inc=1, device_id=(leaf_of[0], my_kv), device_id_type=MESH)
        send_table()

    for role, column, plane in ((is_leaf, leaf_column, leaf_plane), (is_hub, hub_column, hub_plane)):

        @pl.when(jnp.logical_and(role, jnp.logical_not(is_early)))
        def _():
            column(False)
            plane()

        @pl.when(jnp.logical_and(role, is_early))
        def _():
            plane()
            column(True)

    for copy in small[2:]:
        copy.start()
    for s in range(slots):
        pltpu.make_async_copy(key_hbm.at[s], keys.at[s], page_sem.at[0]).start()
        pltpu.make_async_copy(value_hbm.at[s], values.at[s], page_sem.at[1]).start()
    for copy in small[2:]:
        copy.wait()

    homes = []
    for d in range(n_chip):
        pair = []
        for b in range(CORES):
            index, present = jnp.int32(0), jnp.int32(0)
            for s in range(slots):
                same = lax.div(owner_ref[s], group) == d * CORES + b
                index = jnp.where(same, jnp.int32(s), index)
                present = jnp.where(same, jnp.int32(1), present)
            limit = length_ref[owner_ref[index]] - number_ref[index] * page_tokens
            place = jnp.where(present == 1, owner_ref[index] - (d * CORES + b) * group, -1)
            pair.append((index, limit * present, place))
        homes.append(pair)

    edges = sorted({n_chip * k // 4 for k in range(5)})
    alone = [jnp.logical_and(is_hub, my_chip == c) for c in range(n_chip)]
    met = [jnp.logical_not(own) for own in alone]

    @pl.when(is_hub)
    def _():
        q_col[(CORES - 1) * n_kv + my_kv] = q_own[...]
        arrived(q_col, CORES * n_kv - 2, qr_sem.at[0])

        @pl.when(jnp.logical_not(is_early))
        def _():
            arrived(q_col, 1, qr_sem.at[1])

        choices = [q_col[c].astype(jnp.float32) for c in range(CORES * group)]
        for d in range(n_chip - 1, -1, -1):
            arrived(table, CORES if d else CORES - 1, tr_sem.at[d])
            picks = {}
            for a in range(CORES):
                row = table[leaf_of[d] + a]
                for b in range(CORES):
                    rel = row - ((leaf_of[0] + b) * group).astype(jnp.float32)
                    inside = jnp.logical_and(rel >= 0.0, rel < float(group))
                    picks[a, b] = jnp.max(jnp.where(inside, rel, -1.0), axis=1, keepdims=True)
            for a in range(CORES):
                for b in range(CORES):
                    held[b, leaf_of[d] + a] = jnp.broadcast_to(picks[a, b], (1, HEAD_SIZE))
                    pick = jnp.broadcast_to(picks[a, b], (HQ, HEAD_SIZE))
                    chosen = jnp.zeros((HQ, HEAD_SIZE), jnp.float32)
                    for c in range(group):
                        chosen = jnp.where(pick == float(c), choices[b * group + c], chosen)
                    if d == 0 and a == CORES - 1:
                        q_in[my_chip, b] = chosen.astype(jnp.bfloat16)
                    else:
                        q_send[d * CORES + a, b] = chosen.astype(jnp.bfloat16)
                if d or a < CORES - 1:
                    remote(
                        q_send.at[d * CORES + a], q_in.at[my_chip], ds_sem.at[0], dr_sem.at[my_chip],
                        (leaf_of[d] + a, my_kv),
                    ).start()

    pltpu.make_async_copy(key_hbm, keys, page_sem.at[0]).wait()
    pltpu.make_async_copy(value_hbm, values, page_sem.at[1]).wait()

    row = lax.broadcasted_iota(jnp.int32, (HQ, HEAD_SIZE), 0)
    lane = lax.broadcasted_iota(jnp.int32, (HQ, HEAD_SIZE), 1)
    on_diagonal = row == lane
    first = lax.broadcasted_iota(jnp.int32, (PAIR, HEAD_SIZE), 0) < QUERY_PER_KV
    token = lax.broadcasted_iota(jnp.int32, (HQ, page_tokens), 1)
    wide = 2 * HEAD_SIZE

    for stage, (low, high) in enumerate(zip(edges[:-1], edges[1:])):
        batch = [(c, b) for c in range(low, high) for b in range(CORES)]
        for c in range(low, high):

            @pl.when(met[c])
            def _():
                arrived(q_in, 1, dr_sem.at[c])

        scored = {}
        for d, b in batch:
            index, limit, _ = homes[d][b]
            query = q_in[d, b].astype(jnp.float32)
            pieces = []
            for k in range(HQ // PAIR):
                q8 = query[k * PAIR : (k + 1) * PAIR]
                both = jnp.concatenate(
                    [jnp.where(first, q8, 0.0), jnp.where(first, 0.0, q8)], axis=1
                ).astype(jnp.bfloat16)
                pieces.append(
                    lax.dot_general(
                        both, keys[index, :, k * wide : (k + 1) * wide],
                        (((1,), (1,)), ((), ())), preferred_element_type=jnp.float32,
                    )
                )
            scores = jnp.concatenate(pieces, axis=0) * HEAD_SIZE ** (-0.5)
            scored[d, b] = jnp.where(token < limit, scores, lowest)
        tops = {e: jnp.max(scored[e], axis=1, keepdims=True) for e in batch}
        weights = {e: jnp.exp(scored[e] - tops[e]) for e in batch}
        totals = {e: jnp.sum(weights[e], axis=1, keepdims=True) for e in batch}
        summed, largest = {}, {}
        for d, b in batch:
            index, _, _ = homes[d][b]
            blocks = []
            for k in range(HQ // PAIR):
                w8 = weights[d, b][k * PAIR : (k + 1) * PAIR].astype(jnp.bfloat16)
                both = jnp.dot(
                    w8, values[index, :, k * wide : (k + 1) * wide], preferred_element_type=jnp.float32
                )
                blocks.append(jnp.where(first, both[:, :HEAD_SIZE], both[:, HEAD_SIZE:]))
            blocks = jnp.concatenate(blocks, axis=0)
            largest[d, b] = jnp.maximum(jnp.max(jnp.abs(blocks), axis=1, keepdims=True), finest)
            summed[d, b] = blocks
        for d, b in batch:
            coded = jnp.round(summed[d, b] * (1.0 / largest[d, b]) * STEPS)
            part_send[d, b] = coded.astype(jnp.int32).astype(jnp.int16)
            lanes = [diagonal_to_lanes(column[d, b], on_diagonal) for column in (tops, totals, largest)]
            stat_send[d, b] = jnp.concatenate(lanes, axis=0)
            lanes[0] = jnp.where(homes[d][b][2] == 0, lanes[0], lowest)
            near_send[d, b] = jnp.concatenate(lanes, axis=0)
            if b < CORES - 1:
                continue
            target = (d * CORES + CORES - 1, my_kv)
            copy = remote(part_send.at[d], part_in.at[my_req], ps_sem.at[0], pr_sem.at[0], target)
            stat_copy = remote(stat_send.at[d], stat_in.at[my_req], ss_sem.at[0], sr_sem.at[0], target)

            for plane, chips in enumerate((n_chip, n_second)):
                if d >= chips:
                    continue

                @pl.when(my_kv == n_kv - 1 - plane)
                def _():
                    for a in range(CORES):
                        owner, e, k = (d * CORES + a, 0), plane * n_req + my_req, 2 * plane
                        remote(near_send.at[d, a], near_stat.at[e], ns_sem.at[k], nr_sem.at[k], owner).start()
                        remote(part_send.at[d, a], near_in.at[e], ns_sem.at[k + 1], nr_sem.at[k + 1], owner).start()

            @pl.when(met[d])
            def _():
                stat_copy.start()
                copy.start()


    sends_near = jnp.logical_or(is_last, jnp.logical_and(is_relay, my_chip < n_second))

    def send_merged(b, z):
        skipped = sends_near if z == 0 else jnp.bool_(False)
        if b == CORES - 1:
            skipped = jnp.logical_or(skipped, my_kv == z)

        @pl.when(jnp.logical_not(skipped))
        def _():
            remote(
                merged.at[b * n_kv + z], merged_in.at[my_kv], ms_sem.at[0], mr_sem.at[0], (leaf_of[0] + b, z)
            ).start()

    @pl.when(is_hub)
    def _():
        part_in[my_req] = part_send[my_chip]
        stat_in[my_req] = stat_send[my_chip]
        arrived(stat_in, n_req - 1, sr_sem.at[0])
        arrived(part_in, n_req - 1, pr_sem.at[0])
        for b in range(CORES):
            sources = [part_in.at[e, b] for e in range(n_req)]
            stats = [stat_in.at[e, b] for e in range(n_req)]
            tops = [stat[0:1, :] for stat in stats]
            totals = [stat[1:2, :] for stat in stats]
            scales = [stat[2:3, :] for stat in stats]
            picks = [held[b, e] for e in range(n_req)]
            member = [[picks[e] == float(c) for e in range(n_req)] for c in range(group)]
            merged_top, merged_total = [], []
            for c in range(group):
                best = jnp.full((1, HEAD_SIZE), lowest, jnp.float32)
                for e in range(n_req):
                    best = jnp.maximum(best, jnp.where(member[c][e], tops[e], lowest))
                merged_top.append(best)
            factors = []
            for e in range(n_req):
                best = tops[e]
                for c in range(group):
                    best = jnp.where(member[c][e], merged_top[c], best)
                factors.append(jnp.exp(tops[e] - best))
            for c in range(group):
                amount = jnp.zeros((1, HEAD_SIZE), jnp.float32)
                for e in range(n_req):
                    amount = amount + jnp.where(member[c][e], factors[e] * totals[e], 0.0)
                merged_total.append(amount)
            sums = [jnp.zeros((HQ, HEAD_SIZE), jnp.float32) for _ in range(group)]
            for e in range(n_req):
                coded = sources[e][...].astype(jnp.int32).astype(jnp.float32) * (1.0 / STEPS)
                scaled = lanes_to_column(factors[e] * scales[e], on_diagonal) * coded
                pick = jnp.broadcast_to(picks[e], (HQ, HEAD_SIZE))
                for c in range(group):
                    sums[c] = sums[c] + jnp.where(pick == float(c), scaled, 0.0)
            for c in range(group):
                merged[b * n_kv + c, 0:HQ, :] = sums[c]
                merged[b * n_kv + c, HQ : HQ + 2, :] = jnp.concatenate([merged_top[c], merged_total[c]], axis=0)
            send_merged(b, 0)

        for z in range(1, n_kv):
            for b in range(CORES):
                send_merged(b, z)
        merged_in[my_kv] = merged[(CORES - 1) * n_kv + my_kv]

    for role, others in ((is_leaf, n_kv), (is_hub, n_kv - 1)):

        @pl.when(jnp.logical_and(role, jnp.logical_not(is_near)))
        def _():
            arrived(merged_in, others, mr_sem.at[0])

        @pl.when(jnp.logical_and(role, jnp.logical_and(is_near, jnp.logical_not(is_nearest))))
        def _():
            arrived(merged_in, others - 1, mr_sem.at[0])

        @pl.when(jnp.logical_and(role, is_nearest))
        def _():
            arrived(merged_in, others - 2, mr_sem.at[0])

    def merge_near(plane):
        arrived(near_stat, n_req, nr_sem.at[2 * plane])
        some = range(plane * n_req, (plane + 1) * n_req)
        tops = {e: near_stat[e, 0:1, :] for e in some}
        best = functools.reduce(jnp.maximum, tops.values())
        factors = {e: jnp.exp(tops[e] - best) for e in some}
        amount = jnp.zeros((1, HEAD_SIZE), jnp.float32)
        for e in some:
            amount = amount + factors[e] * near_stat[e, 1:2, :]
        arrived(near_in, n_req, nr_sem.at[2 * plane + 1])
        total = jnp.zeros((HQ, HEAD_SIZE), jnp.float32)
        for e in some:
            coded = near_in[e].astype(jnp.int32).astype(jnp.float32) * (1.0 / STEPS)
            total = total + lanes_to_column(factors[e] * near_stat[e, 2:3, :], on_diagonal) * coded
        merged_in[n_kv - 1 - plane, 0:HQ, :] = total
        merged_in[n_kv - 1 - plane, HQ : HQ + 2, :] = jnp.concatenate([best, amount], axis=0)

    @pl.when(is_nearest)
    def _():
        merge_near(1)

    @pl.when(is_near)
    def _():
        merge_near(0)

    tops = [merged_in[c, HQ : HQ + 1, :] for c in range(n_kv)]
    best = tops[0]
    for c in range(1, n_kv):
        best = jnp.maximum(best, tops[c])
    factors = [jnp.exp(tops[c] - best) for c in range(n_kv)]
    amount = jnp.zeros((1, HEAD_SIZE), jnp.float32)
    for c in range(n_kv):
        amount = amount + factors[c] * merged_in[c, HQ + 1 : HQ + 2, :]
    result = jnp.zeros((HQ, HEAD_SIZE), jnp.float32)
    for c in range(n_kv):
        result = result + lanes_to_column(factors[c], on_diagonal) * merged_in[c, 0:HQ, :]
    result = result / lanes_to_column(amount, on_diagonal)
    out_ref[...] = result.astype(jnp.bfloat16)

    for early, leaf_sent, hub_sent in ((True, n_kv - 1, n_kv), (False, n_kv, n_kv - 1)):
        now = is_early if early else jnp.logical_not(is_early)

        @pl.when(jnp.logical_and(is_leaf, now))
        def _():
            arrived(q_col, leaf_sent, qs_sem.at[0])

        @pl.when(jnp.logical_and(is_hub, now))
        def _():
            arrived(q_col, hub_sent, qs_sem.at[0])

    @pl.when(is_leaf)
    def _():
        arrived(table, n_chip, ts_sem.at[0])
        arrived(part_send, n_chip, ps_sem.at[0])
        arrived(stat_send, n_chip, ss_sem.at[0])

    @pl.when(is_hub)
    def _():
        arrived(table, n_chip - 1, ts_sem.at[0])
        arrived(part_send, n_chip - 1, ps_sem.at[0])
        arrived(stat_send, n_chip - 1, ss_sem.at[0])
        arrived(q_send, n_req - 1, ds_sem.at[0])

    @pl.when(jnp.logical_and(is_hub, jnp.logical_not(sends_near)))
    def _():
        arrived(merged, CORES * n_kv - 1, ms_sem.at[0])

    @pl.when(jnp.logical_and(is_hub, sends_near))
    def _():
        arrived(merged, CORES * n_kv - 1 - CORES, ms_sem.at[0])

    for plane, chips in enumerate((n_chip, n_second)):

        @pl.when(my_kv == n_kv - 1 - plane)
        def _():
            arrived(near_send, chips, ns_sem.at[2 * plane])
            arrived(part_send, chips, ns_sem.at[2 * plane + 1])


def solution(mesh):
    n_req, n_kv = mesh.shape["req"], mesh.shape["kv"]

    def on_device(queries, key_cache, value_cache, page_request, page_number, lengths):
        slots, page_tokens, width = key_cache.shape
        group = lengths.shape[0] // n_req
        n_chip = n_req // CORES
        dma = pltpu.SemaphoreType.DMA
        vmem = pl.BlockSpec(memory_space=pltpu.VMEM)
        anywhere = pl.BlockSpec(memory_space=pl.ANY)
        blob = (HQ + 2, HEAD_SIZE)
        attended = pl.pallas_call(
            functools.partial(kernel, n_req, n_kv, group),
            out_shape=pltpu.VMEM((HQ, HEAD_SIZE), jnp.bfloat16),
            in_specs=[anywhere] * 6,
            out_specs=vmem,
            scratch_shapes=[
                pltpu.SMEM(page_request.shape, jnp.int32),
                pltpu.SMEM(page_number.shape, jnp.int32),
                pltpu.SMEM(lengths.shape, jnp.int32),
                pltpu.VMEM(queries.shape, queries.dtype),
                pltpu.VMEM((slots, page_tokens, width), jnp.bfloat16),
                pltpu.VMEM((slots, page_tokens, width), jnp.bfloat16),
                pltpu.VMEM((HQ, HEAD_SIZE), jnp.float32),
                pltpu.VMEM((HQ, HEAD_SIZE), jnp.bfloat16),
                pltpu.VMEM((CORES * n_kv, HQ, HEAD_SIZE), jnp.bfloat16),
                pltpu.VMEM((n_req, 1, HEAD_SIZE), jnp.float32),
                pltpu.VMEM((CORES, n_req, 1, HEAD_SIZE), jnp.float32),
                pltpu.VMEM((n_req, CORES, HQ, HEAD_SIZE), jnp.bfloat16),
                pltpu.VMEM((n_chip, CORES, HQ, HEAD_SIZE), jnp.bfloat16),
                pltpu.VMEM((n_chip, CORES, HQ, HEAD_SIZE), jnp.int16),
                pltpu.VMEM((n_req, CORES, HQ, HEAD_SIZE), jnp.int16),
                pltpu.VMEM((n_chip, CORES, 3, HEAD_SIZE), jnp.float32),
                pltpu.VMEM((n_req, CORES, 3, HEAD_SIZE), jnp.float32),
                pltpu.VMEM((n_chip, CORES, 3, HEAD_SIZE), jnp.float32),
                pltpu.VMEM((2 * n_req, HQ, HEAD_SIZE), jnp.int16),
                pltpu.VMEM((2 * n_req, 3, HEAD_SIZE), jnp.float32),
                pltpu.VMEM((CORES * n_kv,) + blob, jnp.float32),
                pltpu.VMEM((n_kv,) + blob, jnp.float32),
                pltpu.SemaphoreType.REGULAR,
                pltpu.SemaphoreType.REGULAR,
                dma((4,)),
                dma((2,)),
                dma((1,)), dma((2,)),
                dma((1,)), dma((n_chip,)),
                dma((1,)), dma((n_chip,)),
                dma((1,)), dma((1,)),
                dma((1,)), dma((1,)),
                dma((4,)), dma((4,)),
                dma((1,)), dma((1,)),
            ],
            compiler_params=pltpu.CompilerParams(collective_id=0, has_side_effects=True),
        )(page_request, page_number, lengths, queries, key_cache, value_cache)
        return attended.reshape(queries.shape)

    placed = (
        P(("req", "kv"), None),
        P(("req", "kv"), None, None),
        P(("req", "kv"), None, None),
        P(("req", "kv")),
        P(("req", "kv")),
        P(),
    )
    return jax.shard_map(
        on_device, mesh=mesh, in_specs=placed, out_specs=P(("req", "kv"), None), check_vma=False
    )
```
